32 devices in a mesh: batch: 1 (over z), col: 32 (over y, x, core).
Axes of the slice: x: 4, y: 4, z: 1, core: 2. Of those that a mesh axis runs over, the one named last changes fastest.
The devices are a block of a 4x4x8 slice.
Arguments:
- lower: bfloat16 [8192, 8192], P('batch', 'col')
- rhs: bfloat16 [8192, 32768], P('batch', 'col')
Outputs:
- output: bfloat16 [8192, 32768], P('batch', 'col')
All inputs are finite; a program needn't handle non-finite values.
Results may differ from the reference program's by a relative error of at most 0.001.
Values are sent between devices in bfloat16 or wider.
A program may use at most 768 MiB of HBM per device.

```python
import jax
import jax.numpy as jnp
from jax import lax

N = 8192
BLOCK_SIZE = 256
GROUP = 32
COLS_DEV = 1024

PER_DEV = N // (BLOCK_SIZE * GROUP)
COLUMNS = COLS_DEV * GROUP


def setup_inputs(seed: int = 0, part: int = 0) -> dict:
    base_key = jax.random.fold_in(jax.random.key(seed), part)
    key_lower, key_rhs = jax.random.split(base_key)
    entries = jax.random.normal(key_lower, (N, N), jnp.float32)
    natural = jnp.tril(entries) * (N ** -0.5)
    stored = natural.reshape(N, PER_DEV, GROUP, BLOCK_SIZE).transpose(0, 2, 1, 3).reshape(N, N)
    rhs = jax.random.normal(key_rhs, (N, COLUMNS), jnp.float32)
    return {"lower": stored.astype(jnp.bfloat16), "rhs": rhs.astype(jnp.bfloat16)}


def reference(lower, rhs):
    natural = lower.reshape(N, GROUP, PER_DEV, BLOCK_SIZE).transpose(0, 2, 1, 3).reshape(N, N)
    col_groups = rhs.reshape(N, GROUP, COLS_DEV).transpose(1, 0, 2)

    def one_group(rhs_cols):
        return jnp.dot(natural, rhs_cols, preferred_element_type=jnp.float32).astype(jnp.bfloat16)

    results = lax.map(one_group, col_groups)
    return results.transpose(1, 0, 2).reshape(N, COLUMNS)
```

```python
import functools
import math

import jax
import jax.numpy as jnp
from jax import lax
from jax.experimental import pallas as pl
from jax.experimental.pallas import tpu as pltpu
from jax.sharding import PartitionSpec as P

MESH = pl.DeviceIdType.MESH
OFFS = (0, -1, 1, 2)


def kernel(side, l_ref, b_ref, y_ref, g_ref, b_vm, acc, l_vm, st_x, st_y, out_st,
           own_sem, par_sem, send_sem, loc_sem, fold_sem, load_sem, stx_sem, sty_sem, out_sem):
    rows, blk = l_ref.shape
    cols = b_ref.shape[1]
    per_row = 2 * side
    n_part = per_row
    n_full = (side - 1) * per_row // 2
    n_slot = n_part + n_full
    n_iter = n_slot // 2
    me = lax.axis_index("col")
    k = lax.rem(me, 2)
    x = lax.rem(me // 2, side)
    y = me // (2 * side)

    def wrap(v):
        return lax.rem(v + 2 * side, side)

    def dev(yy, xx, kk):
        return {"col": (yy * side + xx) * 2 + kk}

    def where3(c, a, b):
        return jnp.where(c, a, b)

    def strip_of(r, yy):
        f = r - n_part
        full_strip = where3(yy < 2, 20 + f, where3(yy == 2, where3(f < 8, 24 + f, 8 + f), 8 + f))
        full_grp = where3(yy == 0, 0, where3(yy == 1, 1, where3(yy == 2, where3(f < 8, 2, 1), 0)))
        part = r < n_part
        return where3(part, per_row * yy + per_row - 1 - r, full_strip), where3(part, yy, full_grp)

    def exists(r, xx, kk):
        return (r >= n_part) | (2 * xx + kk <= per_row - 1 - r)

    def chunk(r, yy, xx, kk):
        return g_ref.at[r, yy, :, pl.ds(pl.multiple_of((2 * xx + kk) * blk, blk), blk)]

    def pos(first_x, da, db):
        return (wrap(y + db), wrap(x + da)) if first_x else (wrap(y + da), wrap(x + db))

    def plus_dir(is_x, t, src):
        alt = lax.rem(t + src, 2) == 0
        if is_x:
            return alt
        return jnp.where(src == 1, lax.rem(t, 3) != 0, alt)

    def rcopy(r, yy, xx, dst, s, to_partner=False):
        c = chunk(r, yy, xx, k)
        rs = par_sem if to_partner else own_sem
        return pltpu.make_async_remote_copy(
            src_ref=c, dst_ref=c, send_sem=send_sem.at[r, s], recv_sem=rs.at[r, yy * side + xx],
            device_id=dst, device_id_type=MESH)

    def wait_own(r, yy, xx):
        rcopy(r, yy, xx, dev(y, x, k), 0).wait_recv()

    def wait_par(r, yy, xx):
        c = chunk(r, yy, xx, 1 - k)
        pltpu.make_async_copy(c, c, par_sem.at[r, yy * side + xx]).wait()

    def wait_sent(r, s, n):
        c = g_ref.at[0, 0, :, pl.ds(0, n * blk)]
        pltpu.make_async_copy(c, c, send_sem.at[r, s]).wait()

    def neighbour(first_x, first_axis, d):
        on_x = first_x == first_axis
        return dev(y, wrap(x + d), k) if on_x else dev(wrap(y + d), x, k)

    partner = dev(y, x, 1 - k)

    def own_local(r):
        return (r < n_part) | (y < 2) | ((y == 2) & (r < n_part + 8))

    def local_copy(r):
        strip, _ = strip_of(r, y)
        return pltpu.make_async_copy(
            l_vm.at[pl.ds(pl.multiple_of(strip * blk, blk), blk), :], chunk(r, y, x, k), loc_sem.at[r])

    def inject(t):
        for first_x in (True, False):
            r = 2 * t + (0 if first_x else 1)

            @pl.when(exists(r, x, k))
            def _():
                @pl.when(own_local(r))
                def _():
                    local_copy(r).wait()

                @pl.when(jnp.logical_not(own_local(r)))
                def _():
                    wait_own(r, y, x)

                for d in (1, -1):
                    rcopy(r, y, x, neighbour(first_x, True, d), 0).start()
                for d in (1, -1):
                    rcopy(r, y, x, neighbour(first_x, False, d), 0).start()
                rcopy(r, y, x, partner, 0, True).start()

    def first_step(t, i):
        for first_x in (True, False):
            r = 2 * t + (0 if first_x else 1)
            yy, xx = pos(first_x, OFFS[i], 0)

            @pl.when(exists(r, xx, k))
            def _():
                wait_own(r, yy, xx)
                if i < 3:
                    src = xx if first_x else yy
                    plus = plus_dir(first_x, t, src)
                    fwd = plus if i == 1 else jnp.logical_not(plus)

                    @pl.when(fwd)
                    def _():
                        rcopy(r, yy, xx, neighbour(first_x, True, 1 if i == 1 else -1), 3 + i).start()
                for d in (1, -1):
                    rcopy(r, yy, xx, neighbour(first_x, False, d), i).start()
                rcopy(r, yy, xx, partner, i, True).start()

    def second_step(t, i):
        for first_x in (True, False):
            r = 2 * t + (0 if first_x else 1)
            for a in range(4):
                yy, xx = pos(first_x, OFFS[a], OFFS[i])

                @pl.when(exists(r, xx, k))
                def _():
                    wait_own(r, yy, xx)
                    if i < 3:
                        src = yy if first_x else xx
                        plus = plus_dir(not first_x, t, src)
                        fwd = plus if i == 1 else jnp.logical_not(plus)

                        @pl.when(fwd)
                        def _():
                            rcopy(r, yy, xx, neighbour(first_x, False, 1 if i == 1 else -1),
                                  6 + 12 + 4 * (i - 1) + a).start()
                    rcopy(r, yy, xx, partner, 6 + 4 * (i - 1) + a, True).start()

    def drain_first(t):
        for first_x in (True, False):
            r = 2 * t + (0 if first_x else 1)

            @pl.when(exists(r, x, k))
            def _():
                wait_sent(r, 0, 5)
            for i in (1, 2, 3):
                yy, xx = pos(first_x, OFFS[i], 0)

                @pl.when(exists(r, xx, k))
                def _():
                    wait_sent(r, i, 3)
                    if i < 3:
                        plus = plus_dir(first_x, t, xx if first_x else yy)

                        @pl.when(plus if i == 1 else jnp.logical_not(plus))
                        def _():
                            wait_sent(r, 3 + i, 1)

    def drain_second(t):
        for first_x in (True, False):
            r = 2 * t + (0 if first_x else 1)
            for i in (1, 2, 3):
                for a in range(4):
                    yy, xx = pos(first_x, OFFS[a], OFFS[i])

                    @pl.when(exists(r, xx, k))
                    def _():
                        wait_sent(r, 6 + 4 * (i - 1) + a, 1)
                        if i < 3:
                            plus = plus_dir(not first_x, t, yy if first_x else xx)

                            @pl.when(plus if i == 1 else jnp.logical_not(plus))
                            def _():
                                wait_sent(r, 6 + 12 + 4 * (i - 1) + a, 1)

    def fold_copy(f):
        r = n_part + f
        strip = 8 + f
        return pltpu.make_async_remote_copy(
            src_ref=l_vm.at[pl.ds(pl.multiple_of(strip * blk, blk), blk), :],
            dst_ref=chunk(r, 3 - y, x, k), send_sem=fold_sem.at[f],
            recv_sem=own_sem.at[r, (3 - y) * side + x],
            device_id=dev(3 - y, x, k), device_id_type=MESH)

    def fold_cond(f):
        return (y == 0) | ((y == 1) & (f >= 8))

    def stage_x(t, i, buf):
        return pltpu.make_async_copy(g_ref.at[2 * t, wrap(y + OFFS[i])], st_x.at[buf], stx_sem.at[buf])

    def stage_y(t, i, buf, yy):
        xx = wrap(x + OFFS[i])
        return pltpu.make_async_copy(
            g_ref.at[2 * t + 1, yy, :, pl.ds(pl.multiple_of(xx * 2 * blk, 2 * blk), 2 * blk)],
            st_y.at[buf, yy], sty_sem.at[buf])

    def push(t, i, buf):
        for first_x in (True, False):
            r = 2 * t + (0 if first_x else 1)
            for a in range(4):
                yy, xx = pos(first_x, OFFS[a], OFFS[i])

                @pl.when(exists(r, xx, 1 - k))
                def _():
                    wait_par(r, yy, xx)
            if first_x:
                stage_x(t, i, buf).start()
            else:
                for yy in range(side):
                    stage_y(t, i, buf, yy).start()

    def add_dot(lhs, row0, n_rows, strip):
        row0 = pl.multiple_of(row0, 2 * blk)
        arow = pl.multiple_of(strip * blk, blk)
        wn = min(256, cols)
        for n in range(cols // wn):
            acc[pl.ds(arow, blk), n * wn:(n + 1) * wn] += jnp.dot(
                lhs, b_vm[pl.ds(row0, n_rows), n * wn:(n + 1) * wn], preferred_element_type=jnp.float32)

    def compute(t, i, buf):
        r = 2 * t
        stage_x(t, i, buf).wait()
        yy = wrap(y + OFFS[i])

        @pl.when(r < n_part)
        def _():
            for m in range(1, per_row):
                @pl.when(m > per_row - 1 - r)
                def _():
                    st_x[buf, :, m * blk:(m + 1) * blk] = jnp.zeros((blk, blk), st_x.dtype)
        strip, grp = strip_of(r, yy)
        add_dot(st_x[buf], grp * (per_row * blk), per_row * blk, strip)

        r = 2 * t + 1
        c = st_y.at[buf]
        pltpu.make_async_copy(c, c, sty_sem.at[buf]).wait()
        xx = wrap(x + OFFS[i])

        @pl.when(r < n_part)
        def _():
            for kk in range(2):
                @pl.when(2 * xx + kk > per_row - 1 - r)
                def _():
                    st_y[buf, :, :, kk * blk:(kk + 1) * blk] = jnp.zeros((side, blk, blk), st_y.dtype)
        for yy in range(side):
            strip, grp = strip_of(r, yy)
            add_dot(st_y[buf, yy], grp * (per_row * blk) + xx * (2 * blk), 2 * blk, strip)

    def out_copy(strip, buf):
        return pltpu.make_async_copy(
            out_st.at[buf], y_ref.at[pl.ds(pl.multiple_of(strip * blk, blk), blk), :], out_sem.at[buf])

    def out_strips(t):
        for s in range(2):
            r = 2 * t + s
            f = r - n_part
            yield 2 * s, where3(r < n_part, per_row - 1 - r, 20 + f), None
            yield 2 * s + 1, 8 + f, r >= n_part

    def emit(t):
        for buf, strip, cond in out_strips(t):
            def go():
                out_st[buf] = acc[pl.ds(pl.multiple_of(strip * blk, blk), blk), :].astype(out_st.dtype)
                out_copy(strip, buf).start()
            if cond is None:
                go()
            else:
                pl.when(cond)(go)

    def emit_wait(t):
        for buf, strip, cond in out_strips(t):
            def go():
                out_copy(strip, buf).wait()
            if cond is None:
                go()
            else:
                pl.when(cond)(go)

    l_load = pltpu.make_async_copy(l_ref, l_vm, load_sem.at[0])
    l_load.start()
    b_load = pltpu.make_async_copy(b_ref, b_vm, load_sem.at[1])
    b_load.start()
    barrier = pltpu.get_barrier_semaphore()
    for d in (dev(y, wrap(x + 1), k), dev(y, wrap(x - 1), k), dev(wrap(y + 1), x, k), dev(wrap(y - 1), x, k), partner):
        pl.semaphore_signal(barrier, inc=1, device_id=d, device_id_type=MESH)
    l_load.wait()

    def start_local(r, _):
        @pl.when(exists(r, x, k) & own_local(r))
        def _():
            local_copy(r).start()
        return 0
    lax.fori_loop(0, n_slot, start_local, 0)
    pl.semaphore_wait(barrier, 5)
    inject(0)
    inject(1)

    def zero(i, _):
        acc[pl.ds(pl.multiple_of(i * blk, blk), blk), :] = jnp.zeros((blk, cols), acc.dtype)
        return 0
    lax.fori_loop(0, rows // blk, zero, 0)
    for i in (1, 2, 3):
        first_step(0, i)
    push(0, 0, 0)
    b_load.wait()

    def body(t, _):
        more1 = t + 1 < n_iter

        @pl.when(t + 2 < n_iter)
        def _():
            inject(t + 2)

        @pl.when(t < n_full // 2)
        def _():
            for s in range(2):
                @pl.when(fold_cond(2 * t + s))
                def _():
                    fold_copy(2 * t + s).start()

        @pl.when(more1)
        def _():
            first_step(t + 1, 1)
            first_step(t + 1, 2)
        second_step(t, 1)
        push(t, 1, 1)

        @pl.when(t == 0)
        def _():
            compute(0, 0, 0)

        @pl.when(t > 0)
        def _():
            compute(t - 1, 3, 0)

            @pl.when(t > 1)
            def _():
                emit_wait(t - 2)
            emit(t - 1)

        @pl.when(more1)
        def _():
            first_step(t + 1, 3)
            push(t + 1, 0, 0)
        compute(t, 1, 1)
        second_step(t, 2)
        push(t, 2, 1)

        @pl.when(more1)
        def _():
            compute(t + 1, 0, 0)
        second_step(t, 3)
        push(t, 3, 0)
        compute(t, 2, 1)
        drain_first(t)

        @pl.when(t > 0)
        def _():
            drain_second(t - 1)
        return 0
    lax.fori_loop(0, n_iter, body, 0)

    compute(n_iter - 1, 3, 0)
    emit_wait(n_iter - 2)
    emit(n_iter - 1)

    def fold_drain(f, _):
        @pl.when(fold_cond(f))
        def _():
            fold_copy(f).wait_send()
        return 0
    lax.fori_loop(0, n_full, fold_drain, 0)
    drain_second(n_iter - 1)
    emit_wait(n_iter - 1)


def solution(mesh):
    group_size = mesh.shape["col"]
    side = math.isqrt(group_size // 2)

    def local_product(l_cols, b_cols):
        rows, blk = l_cols.shape
        cols = b_cols.shape[1]
        per_row = 2 * side
        n_slot = per_row + (side - 1) * per_row // 2
        dma = pltpu.SemaphoreType.DMA
        product, _ = pl.pallas_call(
            functools.partial(kernel, side),
            out_shape=(
                jax.ShapeDtypeStruct((rows, cols), jnp.bfloat16),
                jax.ShapeDtypeStruct((n_slot, side, blk, per_row * blk), jnp.bfloat16),
            ),
            in_specs=[pl.BlockSpec(memory_space=pl.ANY)] * 2,
            out_specs=(pl.BlockSpec(memory_space=pl.ANY),) * 2,
            scratch_shapes=[
                pltpu.VMEM((rows, cols), jnp.bfloat16),
                pltpu.VMEM((rows, cols), jnp.float32),
                pltpu.VMEM((rows, blk), jnp.bfloat16),
                pltpu.VMEM((2, blk, per_row * blk), jnp.bfloat16),
                pltpu.VMEM((2, side, blk, 2 * blk), jnp.bfloat16),
                pltpu.VMEM((4, blk, cols), jnp.bfloat16),
                dma((n_slot, side * side)),
                dma((n_slot, side * side)),
                dma((n_slot, 26)),
                dma((n_slot,)),
                dma((n_slot - per_row,)),
                dma((2,)),
                dma((2,)),
                dma((2,)),
                dma((4,)),
            ],
            compiler_params=pltpu.CompilerParams(
                collective_id=0, has_side_effects=True, vmem_limit_bytes=67043328),
            cost_estimate=pl.CostEstimate(flops=rows * rows * cols, bytes_accessed=4 * rows * cols, transcendentals=0),
        )(l_cols, b_cols)
        return product

    return jax.shard_map(local_product, mesh=mesh, in_specs=(P("batch", "col"), P("batch", "col")), out_specs=P("batch", "col"), check_vma=False)
```

```python
import functools
import math

import jax
import jax.numpy as jnp
from jax import lax
from jax.experimental import pallas as pl
from jax.experimental.pallas import tpu as pltpu
from jax.sharding import PartitionSpec as P

MESH = pl.DeviceIdType.MESH
OFFS = (0, -1, 1, 2)
DIAG = 6
FULL = 12
SLOTS = DIAG + FULL
PAIRS = SLOTS // 2
FULL_PAIR = DIAG // 2
DIAG_WORK = {2: (7, 6, 0), 3: (5, 1), 4: (4,), 5: (3, 2)}
DIAG_ORDER = sum(DIAG_WORK.values(), ())


def diag_place(p, m):
    k, h = m % 2, m // 2
    main = {0: {6: 1, 7: 2, 4: 3, 5: 4, 3: 5}, 1: {7: 2, 6: 3, 5: 4, 4: 5}}[k]
    alt = {0: {0: 3, 1: 4, 2: 5}, 1: {2: 3, 1: 4, 3: 5}}[k]
    if p in main:
        return main[p], h
    return alt[p], 3 - h


def kernel(side, l_ref, b_ref, y_ref, g_ref, b_vm, acc, l_vm, st_x, st_y, st_d, out_st,
           own_sem, far_sem, par_sem, send_sem, loc_sem, fold_sem, xfold_sem, load_sem,
           stx_sem, sty_sem, std_sem, out_sem, outd_sem):
    rows, blk = l_ref.shape
    cols = b_ref.shape[1]
    per_row = 2 * side
    wide = per_row * blk
    me = lax.axis_index("col")
    k = lax.rem(me, 2)
    x = lax.rem(me // 2, side)
    y = me // (2 * side)
    where = jnp.where

    def wrap(v):
        return lax.rem(v + 2 * side, side)

    def dev(yy, xx, kk):
        return {"col": (yy * side + xx) * 2 + kk}

    partner = dev(y, x, 1 - k)

    def full_strip(f, yy):
        strip = where(yy < 2, 20 + f, where((yy == 2) & (f < 8), 24 + f, 8 + f))
        grp = where(yy == 1, 1, where(yy == 2, where(f < 8, 2, 1), 0))
        return strip, grp

    def diag_main(r):
        return x < where(r <= 2, 4, where(r <= 4, 3, 2))

    def diag_strip(r):
        main = where(r == 1, 6, where(r == 2, 7, where(r == 3, 4 + 2 * k, where(r == 4, 5, 3 + k))))
        alt = where(r == 3, 2 * k, where(r == 4, 1, 2 + k))
        return main, alt

    def exists(r, kk):
        return (r >= 2) | ((r == 1) & (kk == 0))

    def chunk(r, yy, xx, kk):
        return g_ref.at[r, yy, kk, xx]

    def pos(first_x, da, db):
        return (wrap(y + db), wrap(x + da)) if first_x else (wrap(y + da), wrap(x + db))

    def plus_dir(is_x, t, src):
        alt = lax.rem(t + src, 2) == 0
        if is_x:
            return alt
        return where(src == 1, lax.rem(t, 3) != 0, alt)

    def neighbour(first_x, first_axis, d):
        on_x = first_x == first_axis
        return dev(y, wrap(x + d), k) if on_x else dev(wrap(y + d), x, k)

    def slots(t):
        return ((True, 2 * t), (False, 2 * t + 1))

    def rcopy(r, yy, xx, dst, s, rsem):
        c = chunk(r, yy, xx, k)
        return pltpu.make_async_remote_copy(
            src_ref=c, dst_ref=c, send_sem=send_sem.at[r, s], recv_sem=rsem,
            device_id=dst, device_id_type=MESH)

    def osem(r, yy, xx):
        return own_sem.at[r, yy * side + xx]

    def wait_n(sem, n):
        c = g_ref.at[pl.ds(0, n), 0, 0, 0]
        pltpu.make_async_copy(c, c, sem).wait()

    def group(r, first_x, i, kk):
        if first_x:
            return g_ref.at[r, wrap(y + OFFS[i]), kk]
        return g_ref.at[r, :, kk, wrap(x + OFFS[i])]

    def to_partner(first_x, r, i):
        c = group(r, first_x, i, k)
        pltpu.make_async_remote_copy(
            src_ref=c, dst_ref=c, send_sem=send_sem.at[r, 5], recv_sem=par_sem.at[r, i],
            device_id=partner, device_id_type=MESH).start()

    def own_local(r):
        return where(r < DIAG, diag_main(r), (y < 2) | ((y == 2) & (r < DIAG + 8)))

    def l_strip(strip):
        return l_vm.at[pl.ds(pl.multiple_of(strip * blk, blk), blk), :]

    def local_copy(r):
        strip = where(r < DIAG, per_row * y + diag_strip(r)[0], full_strip(r - DIAG, y)[0])
        return pltpu.make_async_copy(l_strip(strip), chunk(r, y, x, k), loc_sem.at[r])

    def inject(t):
        for first_x, r in slots(t):
            @pl.when(exists(r, k))
            def _():
                @pl.when(own_local(r))
                def _():
                    local_copy(r).wait()

                @pl.when(jnp.logical_not(own_local(r)))
                def _():
                    wait_n(osem(r, y, x), 1)

                for first_axis in (True, False):
                    for d in (1, -1):
                        rcopy(r, y, x, neighbour(first_x, first_axis, d), 0, osem(r, y, x)).start()

    def first_step(t, i):
        for first_x, r in slots(t):
            yy, xx = pos(first_x, OFFS[i], 0)

            @pl.when(exists(r, k))
            def _():
                wait_n(osem(r, yy, xx), 1)
                if i < 3:
                    plus = plus_dir(first_x, t, xx if first_x else yy)

                    @pl.when(plus if i == 1 else jnp.logical_not(plus))
                    def _():
                        rcopy(r, yy, xx, neighbour(first_x, True, 1 if i == 1 else -1), i, osem(r, yy, xx)).start()
                for d in (1, -1):
                    rcopy(r, yy, xx, neighbour(first_x, False, d), 0, osem(r, yy, xx)).start()
                if i == 3:
                    to_partner(first_x, r, 0)

    def second_step(t):
        for i in (1, 2):
            for first_x, r in slots(t):
                @pl.when(exists(r, k))
                def _():
                    p0, q0 = pos(first_x, 0, OFFS[i])
                    plus = plus_dir(not first_x, t, p0 if first_x else q0)
                    fwd = plus if i == 1 else jnp.logical_not(plus)
                    for a in range(4):
                        yy, xx = pos(first_x, OFFS[a], OFFS[i])
                        wait_n(osem(r, yy, xx), 1)

                        @pl.when(fwd)
                        def _():
                            rcopy(r, yy, xx, neighbour(first_x, False, 1 if i == 1 else -1), 2 + i,
                                  far_sem.at[r]).start()
                    to_partner(first_x, r, i)

    def far_step(t):
        for first_x, r in slots(t):
            @pl.when(exists(r, k))
            def _():
                wait_n(far_sem.at[r], 4)
                to_partner(first_x, r, 3)

    def drain(t):
        for first_x, r in slots(t):
            @pl.when(exists(r, k))
            def _():
                wait_n(send_sem.at[r, 0], 10)
                for i in (1, 2):
                    yy, xx = pos(first_x, OFFS[i], 0)
                    plus = plus_dir(first_x, t, xx if first_x else yy)

                    @pl.when(plus if i == 1 else jnp.logical_not(plus))
                    def _():
                        wait_n(send_sem.at[r, i], 1)
                    yy, xx = pos(first_x, 0, OFFS[i])
                    plus = plus_dir(not first_x, t, yy if first_x else xx)

                    @pl.when(plus if i == 1 else jnp.logical_not(plus))
                    def _():
                        wait_n(send_sem.at[r, 2 + i], 4)
                wait_n(send_sem.at[r, 5], 4 * side)

    def fold_copy(f):
        r = DIAG + f
        return pltpu.make_async_remote_copy(
            src_ref=l_strip(8 + f), dst_ref=chunk(r, 3 - y, x, k), send_sem=fold_sem.at[f],
            recv_sem=osem(r, 3 - y, x), device_id=dev(3 - y, x, k), device_id_type=MESH)

    def fold_cond(f):
        return (y == 0) | ((y == 1) & (f >= 8))

    def xfold(r):
        return pltpu.make_async_remote_copy(
            src_ref=l_strip(per_row * y + diag_strip(r)[1]), dst_ref=chunk(r, y, 3 - x, k),
            send_sem=xfold_sem.at[r], recv_sem=osem(r, y, 3 - x), device_id=dev(y, 3 - x, k), device_id_type=MESH)

    def xfold_cond(r):
        return (x == 0) | ((x == 1) & (r == 5))

    def stage(t, i, buf):
        yy = wrap(y + OFFS[i])
        xx = wrap(x + OFFS[i])
        for kk in range(2):
            for j in range(side):
                pltpu.make_async_copy(
                    g_ref.at[2 * t, yy, kk, j],
                    st_x.at[buf, :, (2 * j + kk) * blk:(2 * j + kk + 1) * blk], stx_sem.at[buf]).start()
                pltpu.make_async_copy(
                    g_ref.at[2 * t + 1, j, kk, xx],
                    st_y.at[buf, j, :, kk * blk:(kk + 1) * blk], sty_sem.at[buf]).start()

    def par_wait(t, i):
        for first_x, r in slots(t):
            @pl.when(exists(r, 1 - k))
            def _():
                wait_n(par_sem.at[r, i], 4)

    def push(t, i, buf):
        par_wait(t, i)

        @pl.when(t >= FULL_PAIR)
        def _():
            stage(t, i, buf)

    def add_dot(lhs, row0, n_rows, strip):
        row0 = pl.multiple_of(row0, 2 * blk)
        arow = pl.multiple_of(strip * blk, blk)
        wn = min(256, cols)
        for n in range(cols // wn):
            acc[pl.ds(arow, blk), n * wn:(n + 1) * wn] += jnp.dot(
                lhs, b_vm[pl.ds(row0, n_rows), n * wn:(n + 1) * wn], preferred_element_type=jnp.float32)

    def compute(t, i, buf):
        c = st_x.at[buf]
        pltpu.make_async_copy(c, c, stx_sem.at[buf]).wait()
        strip, grp = full_strip(2 * t - DIAG, wrap(y + OFFS[i]))
        add_dot(st_x[buf], grp * wide, wide, strip)

        c = st_y.at[buf]
        pltpu.make_async_copy(c, c, sty_sem.at[buf]).wait()
        xx = wrap(x + OFFS[i])
        for yy in range(side):
            strip, grp = full_strip(2 * t + 1 - DIAG, yy)
            add_dot(st_y[buf, yy], grp * wide + xx * (2 * blk), 2 * blk, strip)

    def diag_stage(p, yy, buf):
        for m in range(p + 1):
            r, xx = diag_place(p, m)
            pltpu.make_async_copy(
                g_ref.at[r, yy, m % 2, xx], st_d.at[buf, :, m * blk:(m + 1) * blk], std_sem.at[buf]).start()

    def diag_compute(p):
        n = (p + 1) * blk
        diag_stage(p, 0, 0)

        def one(yy, _):
            buf = lax.rem(yy, 2)

            @pl.when(yy + 1 < side)
            def _():
                diag_stage(p, yy + 1, 1 - buf)
            c = st_d.at[buf, :, pl.ds(0, n)]
            pltpu.make_async_copy(c, c, std_sem.at[buf]).wait()
            add_dot(st_d[buf, :, :n], yy * wide, n, per_row * yy + p)
            return 0
        lax.fori_loop(0, side, one, 0)

    def out_copy(strip, buf, sem):
        return pltpu.make_async_copy(
            out_st.at[buf], y_ref.at[pl.ds(pl.multiple_of(strip * blk, blk), blk), :], sem)

    def put(strip, buf, sem):
        out_st[buf] = acc[pl.ds(pl.multiple_of(strip * blk, blk), blk), :].astype(out_st.dtype)
        out_copy(strip, buf, sem).start()

    def out_strips(t):
        f = 2 * t - DIAG
        return ((0, 20 + f), (1, 8 + f), (2, 21 + f), (3, 9 + f))

    def emit(t):
        for buf, strip in out_strips(t):
            put(strip, buf, out_sem.at[buf])

    def emit_wait(t):
        for buf, strip in out_strips(t):
            out_copy(strip, buf, out_sem.at[buf]).wait()

    l_load = pltpu.make_async_copy(l_ref, l_vm, load_sem.at[0])
    l_load.start()
    b_load = pltpu.make_async_copy(b_ref, b_vm, load_sem.at[1])
    b_load.start()
    barrier = pltpu.get_barrier_semaphore()
    for d in (dev(y, wrap(x + 1), k), dev(y, wrap(x - 1), k), dev(wrap(y + 1), x, k), dev(wrap(y - 1), x, k), partner):
        pl.semaphore_signal(barrier, inc=1, device_id=d, device_id_type=MESH)
    l_load.wait()

    def start_local(r, _):
        @pl.when(exists(r, k) & own_local(r))
        def _():
            local_copy(r).start()
        return 0
    lax.fori_loop(0, SLOTS, start_local, 0)
    pl.semaphore_wait(barrier, 5)
    for r in (3, 4, 5):
        @pl.when(xfold_cond(r))
        def _():
            xfold(r).start()
    inject(0)
    inject(1)

    def zero(i, _):
        acc[pl.ds(pl.multiple_of(i * blk, blk), blk), :] = jnp.zeros((blk, cols), acc.dtype)
        return 0
    lax.fori_loop(0, rows // blk, zero, 0)
    for r in (3, 4, 5):
        @pl.when(xfold_cond(r))
        def _():
            xfold(r).wait_send()
    b_load.wait()

    def body(n, _):
        t = n - 1
        now = (t >= 0) & (t < PAIRS)
        now_full = (t >= FULL_PAIR) & (t < PAIRS)
        before = t >= 1
        before_full = t > FULL_PAIR
        after = t + 1 < PAIRS

        @pl.when((t >= 0) & (t + 2 < PAIRS))
        def _():
            inject(t + 2)

        @pl.when(t + 1 < FULL // 2)
        def _():
            for s in range(2):
                f = 2 * (t + 1) + s

                @pl.when(fold_cond(f))
                def _():
                    fold_copy(f).start()

        @pl.when(after)
        def _():
            first_step(t + 1, 1)
            first_step(t + 1, 2)

        @pl.when(now)
        def _():
            second_step(t)

        @pl.when(before)
        def _():
            far_step(t - 1)

        @pl.when(now)
        def _():
            push(t, 1, 1)

        @pl.when(now_full)
        def _():
            compute(t, 0, 0)

        @pl.when(now)
        def _():
            push(t, 2, 0)

        @pl.when(now_full)
        def _():
            compute(t, 1, 1)

        @pl.when(after)
        def _():
            first_step(t + 1, 3)

        @pl.when(before)
        def _():
            push(t - 1, 3, 1)

        @pl.when(now_full)
        def _():
            compute(t, 2, 0)

        @pl.when(after)
        def _():
            push(t + 1, 0, 0)

        @pl.when(before_full)
        def _():
            compute(t - 1, 3, 1)
        for tt, ps in DIAG_WORK.items():
            @pl.when(t == tt)
            def _():
                for p in ps:
                    diag_compute(p)
                    n_th = DIAG_ORDER.index(p)
                    if n_th:
                        out_copy(DIAG_ORDER[n_th - 1], 4, outd_sem.at[0]).wait()
                    put(p, 4, outd_sem.at[0])

        @pl.when(before_full)
        def _():
            @pl.when(t > FULL_PAIR + 1)
            def _():
                emit_wait(t - 2)
            emit(t - 1)

        @pl.when(before)
        def _():
            drain(t - 1)
        return 0
    lax.fori_loop(0, PAIRS + 2, body, 0)

    def fold_drain(f, _):
        @pl.when(fold_cond(f))
        def _():
            fold_copy(f).wait_send()
        return 0
    lax.fori_loop(0, FULL, fold_drain, 0)
    emit_wait(PAIRS - 1)
    out_copy(DIAG_ORDER[-1], 4, outd_sem.at[0]).wait()


def solution(mesh):
    group_size = mesh.shape["col"]
    side = math.isqrt(group_size // 2)

    def local_product(l_cols, b_cols):
        rows, blk = l_cols.shape
        cols = b_cols.shape[1]
        per_row = 2 * side
        dma = pltpu.SemaphoreType.DMA
        product, _ = pl.pallas_call(
            functools.partial(kernel, side),
            out_shape=(
                jax.ShapeDtypeStruct((rows, cols), jnp.bfloat16),
                jax.ShapeDtypeStruct((SLOTS, side, 2, side, blk, blk), jnp.bfloat16),
            ),
            in_specs=[pl.BlockSpec(memory_space=pl.ANY)] * 2,
            out_specs=(pl.BlockSpec(memory_space=pl.ANY),) * 2,
            scratch_shapes=[
                pltpu.VMEM((rows, cols), jnp.bfloat16),
                pltpu.VMEM((rows, cols), jnp.float32),
                pltpu.VMEM((rows, blk), jnp.bfloat16),
                pltpu.VMEM((2, blk, per_row * blk), jnp.bfloat16),
                pltpu.VMEM((2, side, blk, 2 * blk), jnp.bfloat16),
                pltpu.VMEM((2, blk, per_row * blk), jnp.bfloat16),
                pltpu.VMEM((5, blk, cols), jnp.bfloat16),
                dma((SLOTS, side * side)),
                dma((SLOTS,)),
                dma((SLOTS, 4)),
                dma((SLOTS, 6)),
                dma((SLOTS,)),
                dma((FULL,)),
                dma((DIAG,)),
                dma((2,)),
                dma((2,)),
                dma((2,)),
                dma((2,)),
                dma((4,)),
                dma((1,)),
            ],
            compiler_params=pltpu.CompilerParams(
                collective_id=0, has_side_effects=True, vmem_limit_bytes=67043328),
            cost_estimate=pl.CostEstimate(flops=rows * rows * cols, bytes_accessed=4 * rows * cols, transcendentals=0),
        )(l_cols, b_cols)
        return product

    return jax.shard_map(local_product, mesh=mesh, in_specs=(P("batch", "col"), P("batch", "col")), out_specs=P("batch", "col"), check_vma=False)
```

```python
import functools
import math

import jax
import jax.numpy as jnp
from jax import lax
from jax.experimental import pallas as pl
from jax.experimental.pallas import tpu as pltpu
from jax.sharding import PartitionSpec as P

MESH = pl.DeviceIdType.MESH
OFFS = (0, -1, 1, 2)
DIAG = 6
FULL = 12
SLOTS = DIAG + FULL
PAIRS = SLOTS // 2
FULL_PAIR = DIAG // 2
DIAG_WORK = {4: (7, 6), 5: (5, 4), 6: (1, 0, 3), 7: (2,)}
DIAG_ORDER = sum(DIAG_WORK.values(), ())


def diag_place(p, m):
    k, h = m % 2, m // 2
    main = {0: {6: 1, 7: 2, 4: 3, 5: 4, 3: 5}, 1: {7: 2, 6: 3, 5: 4, 4: 5}}[k]
    alt = {0: {0: 3, 1: 4, 2: 5}, 1: {2: 3, 1: 4, 3: 5}}[k]
    if p in main:
        return main[p], h
    return alt[p], 3 - h


def kernel(side, l_ref, b_ref, y_ref, g_ref, b_vm, acc, l_vm, st_x, st_y, st_d, out_st,
           own_sem, far_sem, par_sem, send_sem, loc_sem, fold_sem, xfold_sem, load_sem,
           stx_sem, sty_sem, std_sem, out_sem, outd_sem):
    rows, blk = l_ref.shape
    cols = b_ref.shape[1]
    per_row = 2 * side
    wide = per_row * blk
    me = lax.axis_index("col")
    k = lax.rem(me, 2)
    x = lax.rem(me // 2, side)
    y = me // (2 * side)
    where = jnp.where

    def wrap(v):
        return lax.rem(v + 2 * side, side)

    def dev(yy, xx, kk):
        return {"col": (yy * side + xx) * 2 + kk}

    partner = dev(y, x, 1 - k)

    def full_strip(f, yy):
        strip = where(yy < 2, 20 + f, where((yy == 2) & (f < 8), 24 + f, 8 + f))
        grp = where(yy == 1, 1, where(yy == 2, where(f < 8, 2, 1), 0))
        return strip, grp

    def diag_main(r):
        return x < where(r <= 2, 4, where(r <= 4, 3, 2))

    def diag_strip(r):
        main = where(r == 1, 6, where(r == 2, 7, where(r == 3, 4 + 2 * k, where(r == 4, 5, 3 + k))))
        alt = where(r == 3, 2 * k, where(r == 4, 1, 2 + k))
        return main, alt

    def exists(r, kk):
        return (r >= 2) | ((r == 1) & (kk == 0))

    def chunk(r, yy, xx, kk):
        return g_ref.at[r, yy, kk, xx]

    def pos(first_x, da, db):
        return (wrap(y + db), wrap(x + da)) if first_x else (wrap(y + da), wrap(x + db))

    def plus_first(t, src):
        return lax.rem(t + src, 2) == 0

    def plus_second(is_x, t, src, a):
        alt = lax.rem(t, 2) == (0 if a in (0, 3) else 1)
        return alt if is_x else where(src == 1, a != 2, alt)

    def neighbour(first_x, first_axis, d):
        on_x = first_x == first_axis
        return dev(y, wrap(x + d), k) if on_x else dev(wrap(y + d), x, k)

    def slots(t):
        return ((True, 2 * t), (False, 2 * t + 1))

    def rcopy(r, yy, xx, dst, s, rsem):
        c = chunk(r, yy, xx, k)
        return pltpu.make_async_remote_copy(
            src_ref=c, dst_ref=c, send_sem=send_sem.at[r, s], recv_sem=rsem,
            device_id=dst, device_id_type=MESH)

    def osem(r, yy, xx):
        return own_sem.at[r, yy * side + xx]

    def wait_n(sem, n):
        c = g_ref.at[pl.ds(0, n), 0, 0, 0]
        pltpu.make_async_copy(c, c, sem).wait()

    def group(r, first_x, i, kk):
        if first_x:
            return g_ref.at[r, wrap(y + OFFS[i]), kk]
        return g_ref.at[r, :, kk, wrap(x + OFFS[i])]

    def to_partner(first_x, r, i):
        c = group(r, first_x, i, k)
        pltpu.make_async_remote_copy(
            src_ref=c, dst_ref=c, send_sem=send_sem.at[r, 3], recv_sem=par_sem.at[r, i],
            device_id=partner, device_id_type=MESH).start()

    def own_local(r):
        return where(r < DIAG, diag_main(r), (y < 2) | ((y == 2) & (r < DIAG + 8)))

    def l_block(strip):
        return l_ref.at[pl.ds(pl.multiple_of(strip * blk, blk), blk), :]

    def own_strip(r):
        return where(r < DIAG, per_row * y + diag_strip(r)[0], full_strip(r - DIAG, y)[0])

    def local_copy(r):
        return pltpu.make_async_copy(
            l_vm.at[pl.ds(pl.multiple_of(own_strip(r) * blk, blk), blk), :], chunk(r, y, x, k), loc_sem.at[r])

    def inject(t):
        for first_x, r in slots(t):
            @pl.when(exists(r, k))
            def _():
                def go(src):
                    for first_axis in (True, False):
                        for d in (1, -1):
                            pltpu.make_async_remote_copy(
                                src_ref=src, dst_ref=chunk(r, y, x, k), send_sem=send_sem.at[r, 0],
                                recv_sem=osem(r, y, x), device_id=neighbour(first_x, first_axis, d),
                                device_id_type=MESH).start()

                @pl.when(own_local(r))
                def _():
                    go(l_block(own_strip(r)))

                @pl.when(jnp.logical_not(own_local(r)))
                def _():
                    wait_n(osem(r, y, x), 1)
                    go(chunk(r, y, x, k))

    def first_step(t, i):
        for first_x, r in slots(t):
            yy, xx = pos(first_x, OFFS[i], 0)

            @pl.when(exists(r, k))
            def _():
                wait_n(osem(r, yy, xx), 1)
                if i < 3:
                    plus = plus_first(t, xx if first_x else yy)

                    @pl.when(plus if i == 1 else jnp.logical_not(plus))
                    def _():
                        rcopy(r, yy, xx, neighbour(first_x, True, 1 if i == 1 else -1), 0, osem(r, yy, xx)).start()
                for d in (1, -1):
                    rcopy(r, yy, xx, neighbour(first_x, False, d), 0, osem(r, yy, xx)).start()
                if i == 3:
                    @pl.when(own_local(r))
                    def _():
                        local_copy(r).wait()
                    to_partner(first_x, r, 0)

    def second_src(first_x, i):
        p0, q0 = pos(first_x, 0, OFFS[i])
        return p0 if first_x else q0

    def second_step(t, i):
        for first_x, r in slots(t):
            @pl.when(exists(r, k))
            def _():
                for a in range(4):
                    yy, xx = pos(first_x, OFFS[a], OFFS[i])
                    wait_n(osem(r, yy, xx), 1)
                    plus = plus_second(not first_x, t, second_src(first_x, i), a)

                    @pl.when(plus if i == 1 else jnp.logical_not(plus))
                    def _():
                        rcopy(r, yy, xx, neighbour(first_x, False, 1 if i == 1 else -1), i, far_sem.at[r]).start()
                to_partner(first_x, r, i)

    def far_step(t):
        for first_x, r in slots(t):
            @pl.when(exists(r, k))
            def _():
                wait_n(far_sem.at[r], 4)
                to_partner(first_x, r, 3)

    def drain(t):
        for first_x, r in slots(t):
            @pl.when(exists(r, k))
            def _():
                wait_n(send_sem.at[r, 0], 11)
                for i in (1, 2):
                    if first_x:
                        odd = second_src(first_x, i) == 1

                        @pl.when(odd)
                        def _():
                            wait_n(send_sem.at[r, i], 3 if i == 1 else 1)

                        @pl.when(jnp.logical_not(odd))
                        def _():
                            wait_n(send_sem.at[r, i], 2)
                    else:
                        wait_n(send_sem.at[r, i], 2)
                wait_n(send_sem.at[r, 3], 4 * side)

    def fold_copy(f):
        r = DIAG + f
        return pltpu.make_async_remote_copy(
            src_ref=l_block(8 + f), dst_ref=chunk(r, 3 - y, x, k), send_sem=fold_sem.at[f],
            recv_sem=osem(r, 3 - y, x), device_id=dev(3 - y, x, k), device_id_type=MESH)

    def fold_cond(f):
        return (y == 0) | ((y == 1) & (f >= 8))

    def xfold(r):
        return pltpu.make_async_remote_copy(
            src_ref=l_block(per_row * y + diag_strip(r)[1]), dst_ref=chunk(r, y, 3 - x, k),
            send_sem=xfold_sem.at[r], recv_sem=osem(r, y, 3 - x), device_id=dev(y, 3 - x, k), device_id_type=MESH)

    def xfold_cond(r):
        return (x == 0) | ((x == 1) & (r == 5))

    def stage(t, i, buf):
        yy = wrap(y + OFFS[i])
        xx = wrap(x + OFFS[i])
        for kk in range(2):
            for j in range(side):
                pltpu.make_async_copy(
                    g_ref.at[2 * t, yy, kk, j],
                    st_x.at[buf, :, (2 * j + kk) * blk:(2 * j + kk + 1) * blk], stx_sem.at[buf]).start()
                pltpu.make_async_copy(
                    g_ref.at[2 * t + 1, j, kk, xx],
                    st_y.at[buf, j, :, kk * blk:(kk + 1) * blk], sty_sem.at[buf]).start()

    def par_wait(t, i):
        for first_x, r in slots(t):
            @pl.when(exists(r, 1 - k))
            def _():
                wait_n(par_sem.at[r, i], 4)

    def push(t, i, buf):
        par_wait(t, i)

        @pl.when(t >= FULL_PAIR)
        def _():
            stage(t, i, buf)

    def add_dot(lhs, row0, n_rows, strip):
        row0 = pl.multiple_of(row0, 2 * blk)
        arow = pl.multiple_of(strip * blk, blk)
        wn = min(256, cols)
        for n in range(cols // wn):
            acc[pl.ds(arow, blk), n * wn:(n + 1) * wn] += jnp.dot(
                lhs, b_vm[pl.ds(row0, n_rows), n * wn:(n + 1) * wn], preferred_element_type=jnp.float32)

    def compute(t, i, buf):
        c = st_x.at[buf]
        pltpu.make_async_copy(c, c, stx_sem.at[buf]).wait()
        strip, grp = full_strip(2 * t - DIAG, wrap(y + OFFS[i]))
        add_dot(st_x[buf], grp * wide, wide, strip)

        c = st_y.at[buf]
        pltpu.make_async_copy(c, c, sty_sem.at[buf]).wait()
        xx = wrap(x + OFFS[i])
        for yy in range(side):
            strip, grp = full_strip(2 * t + 1 - DIAG, yy)
            add_dot(st_y[buf, yy], grp * wide + xx * (2 * blk), 2 * blk, strip)

    def diag_stage(p, yy, buf):
        for m in range(p + 1):
            r, xx = diag_place(p, m)
            pltpu.make_async_copy(
                g_ref.at[r, yy, m % 2, xx], st_d.at[buf, :, m * blk:(m + 1) * blk], std_sem.at[buf]).start()

    def diag_compute(p, following):
        n = (p + 1) * blk

        def one(yy, _):
            buf = lax.rem(yy, 2)

            @pl.when(yy + 1 < side)
            def _():
                diag_stage(p, yy + 1, 1 - buf)
            if following is not None:
                @pl.when(yy + 1 == side)
                def _():
                    diag_stage(following, 0, 1 - buf)
            c = st_d.at[buf, :, pl.ds(0, n)]
            pltpu.make_async_copy(c, c, std_sem.at[buf]).wait()
            add_dot(st_d[buf, :, :n], yy * wide, n, per_row * yy + p)
            return 0
        lax.fori_loop(0, side, one, 0)

    def out_copy(strip, buf, sem):
        return pltpu.make_async_copy(
            out_st.at[buf], y_ref.at[pl.ds(pl.multiple_of(strip * blk, blk), blk), :], sem)

    def put(strip, buf, sem):
        out_st[buf] = acc[pl.ds(pl.multiple_of(strip * blk, blk), blk), :].astype(out_st.dtype)
        out_copy(strip, buf, sem).start()

    def out_strips(t):
        f = 2 * t - DIAG
        return ((0, 20 + f), (1, 8 + f), (2, 21 + f), (3, 9 + f))

    def emit(t):
        for buf, strip in out_strips(t):
            put(strip, buf, out_sem.at[buf])

    def emit_wait(t):
        for buf, strip in out_strips(t):
            out_copy(strip, buf, out_sem.at[buf]).wait()

    l_load = pltpu.make_async_copy(l_ref, l_vm, load_sem.at[0])
    l_load.start()
    b_load = pltpu.make_async_copy(b_ref, b_vm, load_sem.at[1])
    barrier = pltpu.get_barrier_semaphore()
    for d in (dev(y, wrap(x + 1), k), dev(y, wrap(x - 1), k), dev(wrap(y + 1), x, k), dev(wrap(y - 1), x, k), partner):
        pl.semaphore_signal(barrier, inc=1, device_id=d, device_id_type=MESH)
    pl.semaphore_wait(barrier, 5)
    for r in (3, 4, 5):
        @pl.when(xfold_cond(r))
        def _():
            xfold(r).start()
    inject(0)
    inject(1)
    l_load.wait()

    def start_local(r, _):
        @pl.when(exists(r, k) & own_local(r))
        def _():
            local_copy(r).start()
        return 0
    lax.fori_loop(0, SLOTS, start_local, 0)
    b_load.start()

    def zero(i, _):
        acc[pl.ds(pl.multiple_of(i * blk, blk), blk), :] = jnp.zeros((blk, cols), acc.dtype)
        return 0
    lax.fori_loop(0, rows // blk, zero, 0)
    for r in (3, 4, 5):
        @pl.when(xfold_cond(r))
        def _():
            xfold(r).wait_send()
    b_load.wait()

    def body(n, _):
        t = n - 1

        def on(u, fn, lo=0):
            pl.when((u >= lo) & (u < PAIRS))(fn)

        def full(u, fn):
            on(u, fn, FULL_PAIR)

        for tt, ps in DIAG_WORK.items():
            @pl.when(t == tt)
            def _():
                diag_stage(ps[0], 0, 0)
        on(t - 1, lambda: second_step(t - 1, 1))
        on(t - 1, lambda: push(t - 1, 0, 0))
        for tt, ps in DIAG_WORK.items():
            @pl.when(t == tt)
            def _():
                for h, p in enumerate(ps):
                    diag_compute(p, ps[h + 1] if h + 1 < len(ps) else None)
                    n_th = DIAG_ORDER.index(p)
                    if n_th:
                        out_copy(DIAG_ORDER[n_th - 1], 4, outd_sem.at[0]).wait()
                    put(p, 4, outd_sem.at[0])
        on(t - 2, lambda: far_step(t - 2))
        full(t - 3, lambda: compute(t - 3, 3, 1))
        on(t - 1, lambda: second_step(t - 1, 2))
        on(t - 1, lambda: push(t - 1, 1, 1))
        on(t, lambda: first_step(t, 3))

        @pl.when((t >= 0) & (t + 2 < PAIRS))
        def _():
            inject(t + 2)

        @pl.when(t + 1 < FULL // 2)
        def _():
            for h in range(2):
                f = 2 * (t + 1) + h

                @pl.when(fold_cond(f))
                def _():
                    fold_copy(f).start()
        full(t - 1, lambda: compute(t - 1, 0, 0))

        @pl.when(t + 1 < PAIRS)
        def _():
            first_step(t + 1, 1)
            first_step(t + 1, 2)
        on(t - 1, lambda: push(t - 1, 2, 0))
        full(t - 1, lambda: compute(t - 1, 1, 1))
        on(t - 2, lambda: push(t - 2, 3, 1))
        full(t - 1, lambda: compute(t - 1, 2, 0))

        def send_out():
            @pl.when(t - 4 >= FULL_PAIR)
            def _():
                emit_wait(t - 4)
            emit(t - 3)
        full(t - 3, send_out)
        on(t - 2, lambda: drain(t - 2))
        return 0
    lax.fori_loop(0, PAIRS + 4, body, 0)

    def fold_drain(f, _):
        @pl.when(fold_cond(f))
        def _():
            fold_copy(f).wait_send()
        return 0
    lax.fori_loop(0, FULL, fold_drain, 0)
    emit_wait(PAIRS - 1)
    out_copy(DIAG_ORDER[-1], 4, outd_sem.at[0]).wait()


def solution(mesh):
    group_size = mesh.shape["col"]
    side = math.isqrt(group_size // 2)

    def local_product(l_cols, b_cols):
        rows, blk = l_cols.shape
        cols = b_cols.shape[1]
        per_row = 2 * side
        dma = pltpu.SemaphoreType.DMA
        product, _ = pl.pallas_call(
            functools.partial(kernel, side),
            out_shape=(
                jax.ShapeDtypeStruct((rows, cols), jnp.bfloat16),
                jax.ShapeDtypeStruct((SLOTS, side, 2, side, blk, blk), jnp.bfloat16),
            ),
            in_specs=[pl.BlockSpec(memory_space=pl.ANY)] * 2,
            out_specs=(pl.BlockSpec(memory_space=pl.ANY),) * 2,
            scratch_shapes=[
                pltpu.VMEM((rows, cols), jnp.bfloat16),
                pltpu.VMEM((rows, cols), jnp.float32),
                pltpu.VMEM((rows, blk), jnp.bfloat16),
                pltpu.VMEM((2, blk, per_row * blk), jnp.bfloat16),
                pltpu.VMEM((2, side, blk, 2 * blk), jnp.bfloat16),
                pltpu.VMEM((2, blk, per_row * blk), jnp.bfloat16),
                pltpu.VMEM((5, blk, cols), jnp.bfloat16),
                dma((SLOTS, side * side)),
                dma((SLOTS,)),
                dma((SLOTS, 4)),
                dma((SLOTS, 4)),
                dma((SLOTS,)),
                dma((FULL,)),
                dma((DIAG,)),
                dma((2,)),
                dma((2,)),
                dma((2,)),
                dma((2,)),
                dma((4,)),
                dma((1,)),
            ],
            compiler_params=pltpu.CompilerParams(
                collective_id=0, has_side_effects=True, vmem_limit_bytes=67043328),
            cost_estimate=pl.CostEstimate(flops=rows * rows * cols, bytes_accessed=4 * rows * cols, transcendentals=0),
        )(l_cols, b_cols)
        return product

    return jax.shard_map(local_product, mesh=mesh, in_specs=(P("batch", "col"), P("batch", "col")), out_specs=P("batch", "col"), check_vma=False)
```

```python
import functools
import math

import jax
import jax.numpy as jnp
from jax import lax
from jax.experimental import pallas as pl
from jax.experimental.pallas import tpu as pltpu
from jax.sharding import PartitionSpec as P

MESH = pl.DeviceIdType.MESH
OFFS = (0, -1, 1, 2)
DIAG = 6
FULL = 12
SLOTS = DIAG + FULL
PAIRS = SLOTS // 2
FULL_PAIR = DIAG // 2
DIAG_WORK = {4: (7, 6), 5: (5, 4), 6: (1, 0, 3), 7: (2,)}
DIAG_ORDER = sum(DIAG_WORK.values(), ())


def diag_place(p, m):
    k, h = m % 2, m // 2
    main = {0: {6: 1, 7: 2, 4: 3, 5: 4, 3: 5}, 1: {7: 2, 6: 3, 5: 4, 4: 5}}[k]
    alt = {0: {0: 3, 1: 4, 2: 5}, 1: {2: 3, 1: 4, 3: 5}}[k]
    if p in main:
        return main[p], h
    return alt[p], 3 - h


def full_strip(f, yy):
    strip = jnp.where(yy < 2, 20 + f, jnp.where((yy == 2) & (f < 8), 24 + f, 8 + f))
    grp = jnp.where(yy == 1, 1, jnp.where(yy == 2, jnp.where(f < 8, 2, 1), 0))
    return strip, grp


def strip_rows(ref, strip, blk):
    return ref.at[pl.ds(pl.multiple_of(strip * blk, blk), blk), :]


def late_strips(f, yy):
    first = full_strip(f, yy)[0]
    return (first, 21 + f, 9 + f), 28 + 2 * f - first


def kernel(side, l_ref, b_ref, y_ref, part_ref, g_ref, b_vm, acc, l_vm, st_x, st_y, st_d, out_st,
           own_sem, far_sem, par_sem, send_sem, loc_sem, fold_sem, xfold_sem, load_sem,
           stx_sem, sty_sem, std_sem, out_sem, outd_sem, part_sem):
    rows, blk = l_ref.shape
    cols = b_ref.shape[1]
    per_row = 2 * side
    wide = per_row * blk
    me = lax.axis_index("col")
    k = lax.rem(me, 2)
    x = lax.rem(me // 2, side)
    y = me // (2 * side)
    where = jnp.where

    def wrap(v):
        return lax.rem(v + 2 * side, side)

    def dev(yy, xx, kk):
        return {"col": (yy * side + xx) * 2 + kk}

    partner = dev(y, x, 1 - k)

    def diag_main(r):
        return x < where(r <= 2, 4, where(r <= 4, 3, 2))

    def diag_strip(r):
        main = where(r == 1, 6, where(r == 2, 7, where(r == 3, 4 + 2 * k, where(r == 4, 5, 3 + k))))
        alt = where(r == 3, 2 * k, where(r == 4, 1, 2 + k))
        return main, alt

    def exists(r, kk):
        return (r >= 2) | ((r == 1) & (kk == 0))

    def chunk(r, yy, xx, kk):
        return g_ref.at[r, yy, kk, xx]

    def pos(first_x, da, db):
        return (wrap(y + db), wrap(x + da)) if first_x else (wrap(y + da), wrap(x + db))

    def plus_first(t, src):
        return lax.rem(t + src, 2) == 0

    def plus_second(is_x, t, src, a):
        alt = lax.rem(t, 2) == (0 if a in (0, 3) else 1)
        return alt if is_x else where(src == 1, a != 2, alt)

    def neighbour(first_x, first_axis, d):
        on_x = first_x == first_axis
        return dev(y, wrap(x + d), k) if on_x else dev(wrap(y + d), x, k)

    def slots(t):
        return ((True, 2 * t), (False, 2 * t + 1))

    def rcopy(r, yy, xx, dst, s, rsem):
        c = chunk(r, yy, xx, k)
        return pltpu.make_async_remote_copy(
            src_ref=c, dst_ref=c, send_sem=send_sem.at[r, s], recv_sem=rsem,
            device_id=dst, device_id_type=MESH)

    def osem(r, yy, xx):
        return own_sem.at[r, yy * side + xx]

    def wait_n(sem, n):
        c = g_ref.at[pl.ds(0, n), 0, 0, 0]
        pltpu.make_async_copy(c, c, sem).wait()

    def group(r, first_x, i, kk):
        if first_x:
            return g_ref.at[r, wrap(y + OFFS[i]), kk]
        return g_ref.at[r, :, kk, wrap(x + OFFS[i])]

    def to_partner(first_x, r, i):
        c = group(r, first_x, i, k)
        pltpu.make_async_remote_copy(
            src_ref=c, dst_ref=c, send_sem=send_sem.at[r, 3], recv_sem=par_sem.at[r, i],
            device_id=partner, device_id_type=MESH).start()

    def own_local(r):
        return where(r < DIAG, diag_main(r), (y < 2) | ((y == 2) & (r < DIAG + 8)))

    def l_block(strip):
        return l_ref.at[pl.ds(pl.multiple_of(strip * blk, blk), blk), :]

    def own_strip(r):
        return where(r < DIAG, per_row * y + diag_strip(r)[0], full_strip(r - DIAG, y)[0])

    def local_copy(r):
        return pltpu.make_async_copy(
            l_vm.at[pl.ds(pl.multiple_of(own_strip(r) * blk, blk), blk), :], chunk(r, y, x, k), loc_sem.at[r])

    def inject(t):
        for first_x, r in slots(t):
            @pl.when(exists(r, k))
            def _():
                def go(src):
                    for first_axis in (True, False):
                        for d in (1, -1):
                            pltpu.make_async_remote_copy(
                                src_ref=src, dst_ref=chunk(r, y, x, k), send_sem=send_sem.at[r, 0],
                                recv_sem=osem(r, y, x), device_id=neighbour(first_x, first_axis, d),
                                device_id_type=MESH).start()

                @pl.when(own_local(r))
                def _():
                    go(l_block(own_strip(r)))

                @pl.when(jnp.logical_not(own_local(r)))
                def _():
                    wait_n(osem(r, y, x), 1)
                    go(chunk(r, y, x, k))

    def first_step(t, i):
        for first_x, r in slots(t):
            yy, xx = pos(first_x, OFFS[i], 0)

            @pl.when(exists(r, k))
            def _():
                wait_n(osem(r, yy, xx), 1)
                if i < 3:
                    plus = plus_first(t, xx if first_x else yy)

                    @pl.when(plus if i == 1 else jnp.logical_not(plus))
                    def _():
                        rcopy(r, yy, xx, neighbour(first_x, True, 1 if i == 1 else -1), 0, osem(r, yy, xx)).start()
                for d in (1, -1):
                    rcopy(r, yy, xx, neighbour(first_x, False, d), 0, osem(r, yy, xx)).start()
                if i == 3:
                    @pl.when(own_local(r))
                    def _():
                        local_copy(r).wait()
                    to_partner(first_x, r, 0)

    def second_src(first_x, i):
        p0, q0 = pos(first_x, 0, OFFS[i])
        return p0 if first_x else q0

    def second_step(t, i):
        for first_x, r in slots(t):
            @pl.when(exists(r, k))
            def _():
                for a in range(4):
                    yy, xx = pos(first_x, OFFS[a], OFFS[i])
                    wait_n(osem(r, yy, xx), 1)
                    plus = plus_second(not first_x, t, second_src(first_x, i), a)

                    @pl.when(plus if i == 1 else jnp.logical_not(plus))
                    def _():
                        rcopy(r, yy, xx, neighbour(first_x, False, 1 if i == 1 else -1), i, far_sem.at[r]).start()
                to_partner(first_x, r, i)

    def far_step(t):
        for first_x, r in slots(t):
            @pl.when(exists(r, k))
            def _():
                wait_n(far_sem.at[r], 4)
                to_partner(first_x, r, 3)

    def drain(t):
        for first_x, r in slots(t):
            @pl.when(exists(r, k))
            def _():
                wait_n(send_sem.at[r, 0], 11)
                for i in (1, 2):
                    if first_x:
                        odd = second_src(first_x, i) == 1

                        @pl.when(odd)
                        def _():
                            wait_n(send_sem.at[r, i], 3 if i == 1 else 1)

                        @pl.when(jnp.logical_not(odd))
                        def _():
                            wait_n(send_sem.at[r, i], 2)
                    else:
                        wait_n(send_sem.at[r, i], 2)
                wait_n(send_sem.at[r, 3], 4 * side)

    def fold_copy(f):
        r = DIAG + f
        return pltpu.make_async_remote_copy(
            src_ref=l_block(8 + f), dst_ref=chunk(r, 3 - y, x, k), send_sem=fold_sem.at[f],
            recv_sem=osem(r, 3 - y, x), device_id=dev(3 - y, x, k), device_id_type=MESH)

    def fold_cond(f):
        return (y == 0) | ((y == 1) & (f >= 8))

    def xfold(r):
        return pltpu.make_async_remote_copy(
            src_ref=l_block(per_row * y + diag_strip(r)[1]), dst_ref=chunk(r, y, 3 - x, k),
            send_sem=xfold_sem.at[r], recv_sem=osem(r, y, 3 - x), device_id=dev(y, 3 - x, k), device_id_type=MESH)

    def xfold_cond(r):
        return (x == 0) | ((x == 1) & (r == 5))

    def stage(t, i, buf):
        yy = wrap(y + OFFS[i])
        xx = wrap(x + OFFS[i])
        for kk in range(2):
            for j in range(side):
                pltpu.make_async_copy(
                    g_ref.at[2 * t, yy, kk, j],
                    st_x.at[buf, :, (2 * j + kk) * blk:(2 * j + kk + 1) * blk], stx_sem.at[buf]).start()
                pltpu.make_async_copy(
                    g_ref.at[2 * t + 1, j, kk, xx],
                    st_y.at[buf, j, :, kk * blk:(kk + 1) * blk], sty_sem.at[buf]).start()

    def par_wait(t, i):
        for first_x, r in slots(t):
            @pl.when(exists(r, 1 - k))
            def _():
                wait_n(par_sem.at[r, i], 4)

    def push(t, i, buf):
        par_wait(t, i)

        @pl.when(t >= FULL_PAIR)
        def _():
            stage(t, i, buf)

    def add_dot(lhs, row0, n_rows, strip):
        row0 = pl.multiple_of(row0, 2 * blk)
        arow = pl.multiple_of(strip * blk, blk)
        wn = min(256, cols)
        for n in range(cols // wn):
            acc[pl.ds(arow, blk), n * wn:(n + 1) * wn] += jnp.dot(
                lhs, b_vm[pl.ds(row0, n_rows), n * wn:(n + 1) * wn], preferred_element_type=jnp.float32)

    def compute(t, i, buf):
        c = st_x.at[buf]
        pltpu.make_async_copy(c, c, stx_sem.at[buf]).wait()
        strip, grp = full_strip(2 * t - DIAG, wrap(y + OFFS[i]))
        add_dot(st_x[buf], grp * wide, wide, strip)

        c = st_y.at[buf]
        pltpu.make_async_copy(c, c, sty_sem.at[buf]).wait()
        xx = wrap(x + OFFS[i])
        for yy in range(side):
            strip, grp = full_strip(2 * t + 1 - DIAG, yy)
            add_dot(st_y[buf, yy], grp * wide + xx * (2 * blk), 2 * blk, strip)

    def diag_stage(p, yy, buf):
        for m in range(p + 1):
            r, xx = diag_place(p, m)
            pltpu.make_async_copy(
                g_ref.at[r, yy, m % 2, xx], st_d.at[buf, :, m * blk:(m + 1) * blk], std_sem.at[buf]).start()

    def diag_compute(p, following):
        n = (p + 1) * blk

        def one(yy, _):
            buf = lax.rem(yy, 2)

            @pl.when(yy + 1 < side)
            def _():
                diag_stage(p, yy + 1, 1 - buf)
            if following is not None:
                @pl.when(yy + 1 == side)
                def _():
                    diag_stage(following, 0, 1 - buf)
            c = st_d.at[buf, :, pl.ds(0, n)]
            pltpu.make_async_copy(c, c, std_sem.at[buf]).wait()
            add_dot(st_d[buf, :, :n], yy * wide, n, per_row * yy + p)
            return 0
        lax.fori_loop(0, side, one, 0)

    def out_copy(strip, buf, sem):
        return pltpu.make_async_copy(
            out_st.at[buf], y_ref.at[pl.ds(pl.multiple_of(strip * blk, blk), blk), :], sem)

    def put(strip, buf, sem):
        out_st[buf] = acc[pl.ds(pl.multiple_of(strip * blk, blk), blk), :].astype(out_st.dtype)
        out_copy(strip, buf, sem).start()

    def out_strips(t):
        f = 2 * t - DIAG
        return ((0, 20 + f), (1, 8 + f), (2, 21 + f), (3, 9 + f))

    def emit(t):
        for buf, strip in out_strips(t):
            put(strip, buf, out_sem.at[buf])

    def emit_wait(t):
        for buf, strip in out_strips(t):
            out_copy(strip, buf, out_sem.at[buf]).wait()

    l_load = pltpu.make_async_copy(l_ref, l_vm, load_sem.at[0])
    l_load.start()
    b_load = pltpu.make_async_copy(b_ref, b_vm, load_sem.at[1])
    barrier = pltpu.get_barrier_semaphore()
    for d in (dev(y, wrap(x + 1), k), dev(y, wrap(x - 1), k), dev(wrap(y + 1), x, k), dev(wrap(y - 1), x, k), partner):
        pl.semaphore_signal(barrier, inc=1, device_id=d, device_id_type=MESH)
    pl.semaphore_wait(barrier, 5)
    for r in (3, 4, 5):
        @pl.when(xfold_cond(r))
        def _():
            xfold(r).start()
    inject(0)
    inject(1)
    l_load.wait()

    def start_local(r, _):
        @pl.when(exists(r, k) & own_local(r))
        def _():
            local_copy(r).start()
        return 0
    lax.fori_loop(0, SLOTS, start_local, 0)
    b_load.start()

    def zero(i, _):
        acc[pl.ds(pl.multiple_of(i * blk, blk), blk), :] = jnp.zeros((blk, cols), acc.dtype)
        return 0
    lax.fori_loop(0, rows // blk, zero, 0)
    for r in (3, 4, 5):
        @pl.when(xfold_cond(r))
        def _():
            xfold(r).wait_send()
    b_load.wait()

    def body(n, _):
        t = n - 1

        def on(u, fn, lo=0):
            pl.when((u >= lo) & (u < PAIRS))(fn)

        def full(u, fn):
            on(u, fn, FULL_PAIR)

        for tt, ps in DIAG_WORK.items():
            @pl.when(t == tt)
            def _():
                diag_stage(ps[0], 0, 0)
        on(t - 1, lambda: second_step(t - 1, 1))
        on(t - 1, lambda: push(t - 1, 0, 0))
        for tt, ps in DIAG_WORK.items():
            @pl.when(t == tt)
            def _():
                for h, p in enumerate(ps):
                    diag_compute(p, ps[h + 1] if h + 1 < len(ps) else None)
                    n_th = DIAG_ORDER.index(p)
                    if n_th:
                        out_copy(DIAG_ORDER[n_th - 1], 4, outd_sem.at[0]).wait()
                    put(p, 4, outd_sem.at[0])
        on(t - 2, lambda: far_step(t - 2))
        full(t - 3, lambda: compute(t - 3, 3, 1))
        on(t - 1, lambda: second_step(t - 1, 2))
        on(t - 1, lambda: push(t - 1, 1, 1))
        on(t, lambda: first_step(t, 3))

        @pl.when((t >= 0) & (t + 2 < PAIRS))
        def _():
            inject(t + 2)

        @pl.when(t + 1 < FULL // 2)
        def _():
            for h in range(2):
                f = 2 * (t + 1) + h

                @pl.when(fold_cond(f))
                def _():
                    fold_copy(f).start()
        full(t - 1, lambda: compute(t - 1, 0, 0))

        @pl.when(t + 1 < PAIRS)
        def _():
            first_step(t + 1, 1)
            first_step(t + 1, 2)
        on(t - 1, lambda: push(t - 1, 2, 0))
        full(t - 1, lambda: compute(t - 1, 1, 1))
        on(t - 2, lambda: push(t - 2, 3, 1))
        full(t - 1, lambda: compute(t - 1, 2, 0))

        def send_out():
            @pl.when(t - 4 >= FULL_PAIR)
            def _():
                emit_wait(t - 4)
            emit(t - 3)
        full(t - 3, send_out)
        on(t - 2, lambda: drain(t - 2))
        return 0
    lax.fori_loop(0, PAIRS + 2, body, 0)

    last = PAIRS - 1
    late, other = late_strips(2 * last - DIAG, wrap(y + OFFS[3]))
    parts = [pltpu.make_async_copy(strip_rows(acc, v, blk), part_ref.at[h], part_sem.at[h]) for h, v in enumerate(late)]
    for c in parts:
        c.start()
    out_copy(DIAG_ORDER[-1], 4, outd_sem.at[0]).wait()
    put(other, 4, outd_sem.at[0])
    compute(last - 1, 3, 1)
    emit_wait(last - 2)
    emit(last - 1)
    far_step(last)

    def fold_drain(f, _):
        @pl.when(fold_cond(f))
        def _():
            fold_copy(f).wait_send()
        return 0
    lax.fori_loop(0, FULL, fold_drain, 0)
    for c in parts:
        c.wait()
    emit_wait(last - 1)
    out_copy(other, 4, outd_sem.at[0]).wait()
    par_wait(last, 3)
    drain(last)


def finish(side, y_ref, part_ref, g_ref, b_ref, x_ref, move, bx, by, gx, gy, pv, ov,
           in_sem, read_sem, write_sem):
    blk, cols = move.shape[1:]
    n_copy = move.shape[0]
    per_row = 2 * side
    wide = per_row * blk
    me = lax.axis_index("col")
    x = lax.rem(me // 2, side)
    y = me // per_row
    yy = lax.rem(y + 2, side)
    xx = lax.rem(x + 2, side)
    r = SLOTS - 2
    f = r - DIAG
    late, other = late_strips(f, yy)
    grp = full_strip(f, yy)[1]

    loads = [pltpu.make_async_copy(part_ref, pv, in_sem.at[0]),
             pltpu.make_async_copy(b_ref.at[pl.ds(pl.multiple_of(grp * wide, wide), wide), :], bx, in_sem.at[1])]
    for h in range(2):
        loads.append(pltpu.make_async_copy(
            b_ref.at[pl.ds(pl.multiple_of(h * wide + xx * (2 * blk), 2 * blk), 2 * blk), :], by.at[h], in_sem.at[2 + h]))
    for c in loads:
        c.start()
    for kk in range(2):
        for j in range(side):
            pltpu.make_async_copy(
                g_ref.at[r, yy, kk, j], gx.at[:, (2 * j + kk) * blk:(2 * j + kk + 1) * blk], in_sem.at[4]).start()
            pltpu.make_async_copy(
                g_ref.at[r + 1, j, kk, xx], gy.at[j, :, kk * blk:(kk + 1) * blk], in_sem.at[5]).start()

    def moved(i):
        low = 8 + f
        return jnp.where(i < low, i, jnp.where(i < n_copy - 1, i + 2, other))

    def read(i):
        return pltpu.make_async_copy(strip_rows(y_ref, moved(i), blk), move.at[i], read_sem.at[i])

    def write(i):
        return pltpu.make_async_copy(move.at[i], strip_rows(x_ref, moved(i), blk), write_sem.at[i])

    def each(fn):
        def step(i, _):
            fn(i)
            return 0
        lax.fori_loop(0, n_copy, step, 0)

    each(lambda i: read(i).start())
    for c in loads:
        c.wait()
    pltpu.make_async_copy(gx, gx, in_sem.at[4]).wait()
    pltpu.make_async_copy(gy, gy, in_sem.at[5]).wait()
    wn = min(256, cols)

    def dot(lhs, rhs):
        return jnp.dot(lhs, rhs, preferred_element_type=jnp.float32)

    out = [pltpu.make_async_copy(ov.at[h], strip_rows(x_ref, late[h], blk), write_sem.at[n_copy + h]) for h in range(3)]
    for n in range(cols // wn):
        c = slice(n * wn, (n + 1) * wn)
        ov[0, :, c] = (pv[0, :, c] + dot(gx[...], bx[:, c])).astype(ov.dtype)
    out[0].start()
    for h, rows in ((1, ((0, 0), (1, 1))), (2, ((2, 1), (3, 0)))):
        for n in range(cols // wn):
            c = slice(n * wn, (n + 1) * wn)
            ov[h, :, c] = (pv[h, :, c] + sum(dot(gy[a], by[g, :, c]) for a, g in rows)).astype(ov.dtype)
        out[h].start()

    def pass_on(i):
        read(i).wait()
        write(i).start()
    each(pass_on)
    each(lambda i: write(i).wait())
    for c in out:
        c.wait()


def solution(mesh):
    group_size = mesh.shape["col"]
    side = math.isqrt(group_size // 2)

    def local_product(l_cols, b_cols):
        rows, blk = l_cols.shape
        cols = b_cols.shape[1]
        per_row = 2 * side
        dma = pltpu.SemaphoreType.DMA
        n_copy = rows // blk - 3
        params = pltpu.CompilerParams(collective_id=0, has_side_effects=True, vmem_limit_bytes=67043328)
        strips, partial, gathered = pl.pallas_call(
            functools.partial(kernel, side),
            out_shape=(
                jax.ShapeDtypeStruct((rows, cols), jnp.bfloat16),
                jax.ShapeDtypeStruct((3, blk, cols), jnp.float32),
                jax.ShapeDtypeStruct((SLOTS, side, 2, side, blk, blk), jnp.bfloat16),
            ),
            in_specs=[pl.BlockSpec(memory_space=pl.ANY)] * 2,
            out_specs=(pl.BlockSpec(memory_space=pl.ANY),) * 3,
            scratch_shapes=[
                pltpu.VMEM((rows, cols), jnp.bfloat16),
                pltpu.VMEM((rows, cols), jnp.float32),
                pltpu.VMEM((rows, blk), jnp.bfloat16),
                pltpu.VMEM((2, blk, per_row * blk), jnp.bfloat16),
                pltpu.VMEM((2, side, blk, 2 * blk), jnp.bfloat16),
                pltpu.VMEM((2, blk, per_row * blk), jnp.bfloat16),
                pltpu.VMEM((5, blk, cols), jnp.bfloat16),
                dma((SLOTS, side * side)),
                dma((SLOTS,)),
                dma((SLOTS, 4)),
                dma((SLOTS, 4)),
                dma((SLOTS,)),
                dma((FULL,)),
                dma((DIAG,)),
                dma((2,)),
                dma((2,)),
                dma((2,)),
                dma((2,)),
                dma((4,)),
                dma((1,)),
                dma((3,)),
            ],
            compiler_params=params,
            cost_estimate=pl.CostEstimate(flops=rows * rows * cols, bytes_accessed=4 * rows * cols, transcendentals=0),
        )(l_cols, b_cols)
        return pl.pallas_call(
            functools.partial(finish, side),
            out_shape=jax.ShapeDtypeStruct((rows, cols), jnp.bfloat16),
            in_specs=[pl.BlockSpec(memory_space=pl.ANY)] * 4,
            out_specs=pl.BlockSpec(memory_space=pl.ANY),
            scratch_shapes=[
                pltpu.VMEM((n_copy, blk, cols), jnp.bfloat16),
                pltpu.VMEM((per_row * blk, cols), jnp.bfloat16),
                pltpu.VMEM((2, 2 * blk, cols), jnp.bfloat16),
                pltpu.VMEM((blk, per_row * blk), jnp.bfloat16),
                pltpu.VMEM((side, blk, 2 * blk), jnp.bfloat16),
                pltpu.VMEM((3, blk, cols), jnp.float32),
                pltpu.VMEM((3, blk, cols), jnp.bfloat16),
                dma((6,)),
                dma((n_copy,)),
                dma((n_copy + 3,)),
            ],
            compiler_params=pltpu.CompilerParams(vmem_limit_bytes=67043328),
            cost_estimate=pl.CostEstimate(flops=2 * rows * blk * cols, bytes_accessed=6 * rows * cols, transcendentals=0),
        )(strips, partial, gathered, b_cols)

    return jax.shard_map(local_product, mesh=mesh, in_specs=(P("batch", "col"), P("batch", "col")), out_specs=P("batch", "col"), check_vma=False)
```

```python
import functools
import math

import jax
import jax.numpy as jnp
from jax import lax
from jax.experimental import pallas as pl
from jax.experimental.pallas import tpu as pltpu
from jax.sharding import PartitionSpec as P

MESH = pl.DeviceIdType.MESH
OFFS = (0, -1, 1, 2)
DIAG = 6
FULL = 12
SLOTS = DIAG + FULL
PAIRS = SLOTS // 2
FULL_PAIR = DIAG // 2
DIAG_WORK = {4: (7, 6), 5: (5, 4), 6: (1, 0, 3), 7: (2,)}
DIAG_ORDER = sum(DIAG_WORK.values(), ())


def diag_place(p, m):
    k, h = m % 2, m // 2
    main = {0: {6: 1, 7: 2, 4: 3, 5: 4, 3: 5}, 1: {7: 2, 6: 3, 5: 4, 4: 5}}[k]
    alt = {0: {0: 3, 1: 4, 2: 5}, 1: {2: 3, 1: 4, 3: 5}}[k]
    if p in main:
        return main[p], h
    return alt[p], 3 - h


def full_strip(f, yy):
    strip = jnp.where(yy < 2, 20 + f, jnp.where((yy == 2) & (f < 8), 24 + f, 8 + f))
    grp = jnp.where(yy == 1, 1, jnp.where(yy == 2, jnp.where(f < 8, 2, 1), 0))
    return strip, grp


def strip_rows(ref, strip, blk):
    return ref.at[pl.ds(pl.multiple_of(strip * blk, blk), blk), :]


LATE = FULL - 2
LATE_STRIPS = (20 + LATE, 8 + LATE, 21 + LATE, 9 + LATE)


def kernel(side, l_ref, b_ref, y_ref, part_ref, g_ref, b_vm, acc, l_vm, st_x, st_y, st_d, out_st,
           own_sem, far_sem, par_sem, send_sem, loc_sem, fold_sem, xfold_sem, load_sem,
           stx_sem, sty_sem, std_sem, out_sem, outd_sem, part_sem):
    rows, blk = l_ref.shape
    cols = b_ref.shape[1]
    per_row = 2 * side
    wide = per_row * blk
    me = lax.axis_index("col")
    k = lax.rem(me, 2)
    x = lax.rem(me // 2, side)
    y = me // (2 * side)
    where = jnp.where

    def wrap(v):
        return lax.rem(v + 2 * side, side)

    def dev(yy, xx, kk):
        return {"col": (yy * side + xx) * 2 + kk}

    partner = dev(y, x, 1 - k)

    def diag_main(r):
        return x < where(r <= 2, 4, where(r <= 4, 3, 2))

    def diag_strip(r):
        main = where(r == 1, 6, where(r == 2, 7, where(r == 3, 4 + 2 * k, where(r == 4, 5, 3 + k))))
        alt = where(r == 3, 2 * k, where(r == 4, 1, 2 + k))
        return main, alt

    def exists(r, kk):
        return (r >= 2) | ((r == 1) & (kk == 0))

    def chunk(r, yy, xx, kk):
        return g_ref.at[r, yy, kk, xx]

    def pos(first_x, da, db):
        return (wrap(y + db), wrap(x + da)) if first_x else (wrap(y + da), wrap(x + db))

    def plus_first(t, src):
        return lax.rem(t + src, 2) == 0

    def plus_second(is_x, t, src, a):
        alt = lax.rem(t, 2) == (0 if a in (0, 3) else 1)
        return alt if is_x else where(src == 1, a != 2, alt)

    def neighbour(first_x, first_axis, d):
        on_x = first_x == first_axis
        return dev(y, wrap(x + d), k) if on_x else dev(wrap(y + d), x, k)

    def slots(t):
        return ((True, 2 * t), (False, 2 * t + 1))

    def rcopy(r, yy, xx, dst, s, rsem):
        c = chunk(r, yy, xx, k)
        return pltpu.make_async_remote_copy(
            src_ref=c, dst_ref=c, send_sem=send_sem.at[r, s], recv_sem=rsem,
            device_id=dst, device_id_type=MESH)

    def osem(r, yy, xx):
        return own_sem.at[r, yy * side + xx]

    def wait_n(sem, n):
        c = g_ref.at[pl.ds(0, n), 0, 0, 0]
        pltpu.make_async_copy(c, c, sem).wait()

    def group(r, first_x, i, kk):
        if first_x:
            return g_ref.at[r, wrap(y + OFFS[i]), kk]
        return g_ref.at[r, :, kk, wrap(x + OFFS[i])]

    def to_partner(first_x, r, i):
        c = group(r, first_x, i, k)
        pltpu.make_async_remote_copy(
            src_ref=c, dst_ref=c, send_sem=send_sem.at[r, 3], recv_sem=par_sem.at[r, i],
            device_id=partner, device_id_type=MESH).start()

    def own_local(r):
        return where(r < DIAG, diag_main(r), (y < 2) | ((y == 2) & (r < DIAG + 8)))

    def l_block(strip):
        return l_ref.at[pl.ds(pl.multiple_of(strip * blk, blk), blk), :]

    def own_strip(r):
        return where(r < DIAG, per_row * y + diag_strip(r)[0], full_strip(r - DIAG, y)[0])

    def local_copy(r):
        return pltpu.make_async_copy(
            l_vm.at[pl.ds(pl.multiple_of(own_strip(r) * blk, blk), blk), :], chunk(r, y, x, k), loc_sem.at[r])

    def inject(t):
        for first_x, r in slots(t):
            @pl.when(exists(r, k))
            def _():
                def go(src):
                    for first_axis in (True, False):
                        for d in (1, -1):
                            pltpu.make_async_remote_copy(
                                src_ref=src, dst_ref=chunk(r, y, x, k), send_sem=send_sem.at[r, 0],
                                recv_sem=osem(r, y, x), device_id=neighbour(first_x, first_axis, d),
                                device_id_type=MESH).start()

                @pl.when(own_local(r))
                def _():
                    go(l_block(own_strip(r)))

                @pl.when(jnp.logical_not(own_local(r)))
                def _():
                    wait_n(osem(r, y, x), 1)
                    go(chunk(r, y, x, k))

    def first_step(t, i):
        for first_x, r in slots(t):
            yy, xx = pos(first_x, OFFS[i], 0)

            @pl.when(exists(r, k))
            def _():
                wait_n(osem(r, yy, xx), 1)
                if i < 3:
                    plus = plus_first(t, xx if first_x else yy)

                    @pl.when(plus if i == 1 else jnp.logical_not(plus))
                    def _():
                        rcopy(r, yy, xx, neighbour(first_x, True, 1 if i == 1 else -1), 0, osem(r, yy, xx)).start()
                for d in (1, -1):
                    rcopy(r, yy, xx, neighbour(first_x, False, d), 0, osem(r, yy, xx)).start()
                if i == 3:
                    @pl.when(own_local(r))
                    def _():
                        local_copy(r).wait()
                    to_partner(first_x, r, 0)

    def second_src(first_x, i):
        p0, q0 = pos(first_x, 0, OFFS[i])
        return p0 if first_x else q0

    def second_step(t, i):
        for first_x, r in slots(t):
            @pl.when(exists(r, k))
            def _():
                for a in range(4):
                    yy, xx = pos(first_x, OFFS[a], OFFS[i])
                    wait_n(osem(r, yy, xx), 1)
                    plus = plus_second(not first_x, t, second_src(first_x, i), a)

                    @pl.when(plus if i == 1 else jnp.logical_not(plus))
                    def _():
                        rcopy(r, yy, xx, neighbour(first_x, False, 1 if i == 1 else -1), i, far_sem.at[r]).start()
                to_partner(first_x, r, i)

    def far_step(t):
        for first_x, r in slots(t):
            @pl.when(exists(r, k))
            def _():
                wait_n(far_sem.at[r], 4)
                to_partner(first_x, r, 3)

    def drain(t):
        for first_x, r in slots(t):
            @pl.when(exists(r, k))
            def _():
                wait_n(send_sem.at[r, 0], 11)
                for i in (1, 2):
                    if first_x:
                        odd = second_src(first_x, i) == 1

                        @pl.when(odd)
                        def _():
                            wait_n(send_sem.at[r, i], 3 if i == 1 else 1)

                        @pl.when(jnp.logical_not(odd))
                        def _():
                            wait_n(send_sem.at[r, i], 2)
                    else:
                        wait_n(send_sem.at[r, i], 2)
                wait_n(send_sem.at[r, 3], 4 * side)

    def fold_copy(f):
        r = DIAG + f
        return pltpu.make_async_remote_copy(
            src_ref=l_block(8 + f), dst_ref=chunk(r, 3 - y, x, k), send_sem=fold_sem.at[f],
            recv_sem=osem(r, 3 - y, x), device_id=dev(3 - y, x, k), device_id_type=MESH)

    def fold_cond(f):
        return (y == 0) | ((y == 1) & (f >= 8))

    def xfold(r):
        return pltpu.make_async_remote_copy(
            src_ref=l_block(per_row * y + diag_strip(r)[1]), dst_ref=chunk(r, y, 3 - x, k),
            send_sem=xfold_sem.at[r], recv_sem=osem(r, y, 3 - x), device_id=dev(y, 3 - x, k), device_id_type=MESH)

    def xfold_cond(r):
        return (x == 0) | ((x == 1) & (r == 5))

    def stage(t, i, buf):
        yy = wrap(y + OFFS[i])
        xx = wrap(x + OFFS[i])
        for kk in range(2):
            for j in range(side):
                pltpu.make_async_copy(
                    g_ref.at[2 * t, yy, kk, j],
                    st_x.at[buf, :, (2 * j + kk) * blk:(2 * j + kk + 1) * blk], stx_sem.at[buf]).start()
                pltpu.make_async_copy(
                    g_ref.at[2 * t + 1, j, kk, xx],
                    st_y.at[buf, j, :, kk * blk:(kk + 1) * blk], sty_sem.at[buf]).start()

    def par_wait(t, i):
        for first_x, r in slots(t):
            @pl.when(exists(r, 1 - k))
            def _():
                wait_n(par_sem.at[r, i], 4)

    def push(t, i, buf):
        par_wait(t, i)

        @pl.when((t >= FULL_PAIR) & (t < PAIRS - 1))
        def _():
            stage(t, i, buf)

    def add_dot(lhs, row0, n_rows, strip):
        row0 = pl.multiple_of(row0, 2 * blk)
        arow = pl.multiple_of(strip * blk, blk)
        wn = min(256, cols)
        for n in range(cols // wn):
            acc[pl.ds(arow, blk), n * wn:(n + 1) * wn] += jnp.dot(
                lhs, b_vm[pl.ds(row0, n_rows), n * wn:(n + 1) * wn], preferred_element_type=jnp.float32)

    def compute(t, i, buf):
        c = st_x.at[buf]
        pltpu.make_async_copy(c, c, stx_sem.at[buf]).wait()
        strip, grp = full_strip(2 * t - DIAG, wrap(y + OFFS[i]))
        add_dot(st_x[buf], grp * wide, wide, strip)

        c = st_y.at[buf]
        pltpu.make_async_copy(c, c, sty_sem.at[buf]).wait()
        xx = wrap(x + OFFS[i])
        for yy in range(side):
            strip, grp = full_strip(2 * t + 1 - DIAG, yy)
            add_dot(st_y[buf, yy], grp * wide + xx * (2 * blk), 2 * blk, strip)

    def diag_stage(p, yy, buf):
        for m in range(p + 1):
            r, xx = diag_place(p, m)
            pltpu.make_async_copy(
                g_ref.at[r, yy, m % 2, xx], st_d.at[buf, :, m * blk:(m + 1) * blk], std_sem.at[buf]).start()

    def diag_compute(p, following):
        n = (p + 1) * blk

        def one(yy, _):
            buf = lax.rem(yy, 2)

            @pl.when(yy + 1 < side)
            def _():
                diag_stage(p, yy + 1, 1 - buf)
            if following is not None:
                @pl.when(yy + 1 == side)
                def _():
                    diag_stage(following, 0, 1 - buf)
            c = st_d.at[buf, :, pl.ds(0, n)]
            pltpu.make_async_copy(c, c, std_sem.at[buf]).wait()
            add_dot(st_d[buf, :, :n], yy * wide, n, per_row * yy + p)
            return 0
        lax.fori_loop(0, side, one, 0)

    def out_copy(strip, buf, sem):
        return pltpu.make_async_copy(
            out_st.at[buf], y_ref.at[pl.ds(pl.multiple_of(strip * blk, blk), blk), :], sem)

    def put(strip, buf, sem):
        out_st[buf] = acc[pl.ds(pl.multiple_of(strip * blk, blk), blk), :].astype(out_st.dtype)
        out_copy(strip, buf, sem).start()

    def out_strips(t):
        f = 2 * t - DIAG
        return ((0, 20 + f), (1, 8 + f), (2, 21 + f), (3, 9 + f))

    def emit(t):
        for buf, strip in out_strips(t):
            put(strip, buf, out_sem.at[buf])

    def emit_wait(t):
        for buf, strip in out_strips(t):
            out_copy(strip, buf, out_sem.at[buf]).wait()

    l_load = pltpu.make_async_copy(l_ref, l_vm, load_sem.at[0])
    l_load.start()
    b_load = pltpu.make_async_copy(b_ref, b_vm, load_sem.at[1])
    barrier = pltpu.get_barrier_semaphore()
    for d in (dev(y, wrap(x + 1), k), dev(y, wrap(x - 1), k), dev(wrap(y + 1), x, k), dev(wrap(y - 1), x, k), partner):
        pl.semaphore_signal(barrier, inc=1, device_id=d, device_id_type=MESH)
    pl.semaphore_wait(barrier, 5)
    for r in (3, 4, 5):
        @pl.when(xfold_cond(r))
        def _():
            xfold(r).start()
    inject(0)
    inject(1)
    l_load.wait()

    def start_local(r, _):
        @pl.when(exists(r, k) & own_local(r))
        def _():
            local_copy(r).start()
        return 0
    lax.fori_loop(0, SLOTS, start_local, 0)
    b_load.start()

    def zero(i, _):
        acc[pl.ds(pl.multiple_of(i * blk, blk), blk), :] = jnp.zeros((blk, cols), acc.dtype)
        return 0
    lax.fori_loop(0, rows // blk, zero, 0)
    for r in (3, 4, 5):
        @pl.when(xfold_cond(r))
        def _():
            xfold(r).wait_send()
    b_load.wait()

    def body(n, _):
        t = n - 1

        def on(u, fn, lo=0):
            pl.when((u >= lo) & (u < PAIRS))(fn)

        def full(u, fn):
            pl.when((u >= FULL_PAIR) & (u < PAIRS - 1))(fn)

        for tt, ps in DIAG_WORK.items():
            @pl.when(t == tt)
            def _():
                diag_stage(ps[0], 0, 0)
        on(t - 1, lambda: second_step(t - 1, 1))
        on(t - 1, lambda: push(t - 1, 0, 0))
        for tt, ps in DIAG_WORK.items():
            @pl.when(t == tt)
            def _():
                for h, p in enumerate(ps):
                    diag_compute(p, ps[h + 1] if h + 1 < len(ps) else None)
                    n_th = DIAG_ORDER.index(p)
                    if n_th:
                        out_copy(DIAG_ORDER[n_th - 1], 4, outd_sem.at[0]).wait()
                    put(p, 4, outd_sem.at[0])
        on(t - 2, lambda: far_step(t - 2))
        full(t - 3, lambda: compute(t - 3, 3, 1))
        on(t - 1, lambda: second_step(t - 1, 2))
        on(t - 1, lambda: push(t - 1, 1, 1))
        on(t, lambda: first_step(t, 3))

        @pl.when((t >= 0) & (t + 2 < PAIRS))
        def _():
            inject(t + 2)

        @pl.when(t + 1 < FULL // 2)
        def _():
            for h in range(2):
                f = 2 * (t + 1) + h

                @pl.when(fold_cond(f))
                def _():
                    fold_copy(f).start()
        full(t - 1, lambda: compute(t - 1, 0, 0))

        @pl.when(t + 1 < PAIRS)
        def _():
            first_step(t + 1, 1)
            first_step(t + 1, 2)
        on(t - 1, lambda: push(t - 1, 2, 0))
        full(t - 1, lambda: compute(t - 1, 1, 1))
        on(t - 2, lambda: push(t - 2, 3, 1))
        full(t - 1, lambda: compute(t - 1, 2, 0))

        def send_out():
            @pl.when(t - 4 >= FULL_PAIR)
            def _():
                emit_wait(t - 4)
            emit(t - 3)
        full(t - 3, send_out)
        on(t - 2, lambda: drain(t - 2))
        return 0
    lax.fori_loop(0, PAIRS + 2, body, 0)

    last = PAIRS - 1
    parts = [pltpu.make_async_copy(strip_rows(acc, v, blk), part_ref.at[h], part_sem.at[h]) for h, v in enumerate(LATE_STRIPS)]
    for c in parts:
        c.start()
    out_copy(DIAG_ORDER[-1], 4, outd_sem.at[0]).wait()
    compute(last - 1, 3, 1)
    emit_wait(last - 2)
    emit(last - 1)
    far_step(last)

    def fold_drain(f, _):
        @pl.when(fold_cond(f))
        def _():
            fold_copy(f).wait_send()
        return 0
    lax.fori_loop(0, FULL, fold_drain, 0)
    for c in parts:
        c.wait()
    emit_wait(last - 1)
    par_wait(last, 3)
    drain(last)


def finish(side, y_ref, part_ref, g_ref, b_ref, x_ref, move, bv, gv, pv, ov,
           b_sem, g_sem, p_sem, read_sem, write_sem):
    blk, cols = move.shape[1:]
    n_copy = move.shape[0]
    wide = 2 * side * blk
    wn = min(256, cols)
    terms = (((0, 0, 0), (1, 0, 3), (2, 1, 0), (3, 1, 3)), ((0, 0, 1), (1, 0, 2), (2, 1, 1), (3, 1, 2)))

    def load_b(g):
        return pltpu.make_async_copy(b_ref.at[pl.ds(g * wide, wide), :], bv.at[g], b_sem.at[g])

    def load_p(h):
        return pltpu.make_async_copy(part_ref.at[h], pv.at[h], p_sem.at[h])

    def moved(i):
        return jnp.where(i < LATE_STRIPS[1], i, i + 2)

    def read(i):
        return pltpu.make_async_copy(strip_rows(y_ref, moved(i), blk), move.at[i], read_sem.at[i])

    def write(i):
        return pltpu.make_async_copy(move.at[i], strip_rows(x_ref, moved(i), blk), write_sem.at[i])

    def each(lo, hi, fn):
        def step(i, _):
            fn(i)
            return 0
        lax.fori_loop(lo, hi, step, 0)

    per = -(-n_copy // 8)
    n = 0
    for g in range(2):
        load_b(g).start()
        for h, slot, yy in terms[g]:
            for kk in range(2):
                for j in range(side):
                    pltpu.make_async_copy(
                        g_ref.at[SLOTS - 2 + slot, yy, kk, j],
                        gv.at[4 * g + h, :, (2 * j + kk) * blk:(2 * j + kk + 1) * blk], g_sem.at[4 * g + h]).start()
            if g == 0:
                load_p(h).start()
            each(n, min(n + per, n_copy), lambda i: read(i).start())
            n = min(n + per, n_copy)

    def pass_on(i):
        read(i).wait()
        write(i).start()

    n = 0
    for g in range(2):
        load_b(g).wait()
        for h, _, _ in terms[g]:
            c = gv.at[4 * g + h]
            pltpu.make_async_copy(c, c, g_sem.at[4 * g + h]).wait()
            if g == 0:
                load_p(h).wait()
            for m in range(cols // wn):
                c = slice(m * wn, (m + 1) * wn)
                total = pv[h, :, c] + jnp.dot(gv[4 * g + h], bv[g, :, c], preferred_element_type=jnp.float32)
                if g == 0:
                    pv[h, :, c] = total
                else:
                    ov[h, :, c] = total.astype(ov.dtype)
            if g == 1:
                pltpu.make_async_copy(ov.at[h], strip_rows(x_ref, LATE_STRIPS[h], blk), write_sem.at[n_copy + h]).start()
            each(n, min(n + per, n_copy), pass_on)
            n = min(n + per, n_copy)
    each(0, n_copy, lambda i: write(i).wait())
    for h in range(4):
        pltpu.make_async_copy(ov.at[h], strip_rows(x_ref, LATE_STRIPS[h], blk), write_sem.at[n_copy + h]).wait()


def solution(mesh):
    group_size = mesh.shape["col"]
    side = math.isqrt(group_size // 2)

    def local_product(l_cols, b_cols):
        rows, blk = l_cols.shape
        cols = b_cols.shape[1]
        per_row = 2 * side
        dma = pltpu.SemaphoreType.DMA
        n_copy = rows // blk - 4
        params = pltpu.CompilerParams(collective_id=0, has_side_effects=True, vmem_limit_bytes=67043328)
        strips, partial, gathered = pl.pallas_call(
            functools.partial(kernel, side),
            out_shape=(
                jax.ShapeDtypeStruct((rows, cols), jnp.bfloat16),
                jax.ShapeDtypeStruct((4, blk, cols), jnp.float32),
                jax.ShapeDtypeStruct((SLOTS, side, 2, side, blk, blk), jnp.bfloat16),
            ),
            in_specs=[pl.BlockSpec(memory_space=pl.ANY)] * 2,
            out_specs=(pl.BlockSpec(memory_space=pl.ANY),) * 3,
            scratch_shapes=[
                pltpu.VMEM((rows, cols), jnp.bfloat16),
                pltpu.VMEM((rows, cols), jnp.float32),
                pltpu.VMEM((rows, blk), jnp.bfloat16),
                pltpu.VMEM((2, blk, per_row * blk), jnp.bfloat16),
                pltpu.VMEM((2, side, blk, 2 * blk), jnp.bfloat16),
                pltpu.VMEM((2, blk, per_row * blk), jnp.bfloat16),
                pltpu.VMEM((5, blk, cols), jnp.bfloat16),
                dma((SLOTS, side * side)),
                dma((SLOTS,)),
                dma((SLOTS, 4)),
                dma((SLOTS, 4)),
                dma((SLOTS,)),
                dma((FULL,)),
                dma((DIAG,)),
                dma((2,)),
                dma((2,)),
                dma((2,)),
                dma((2,)),
                dma((4,)),
                dma((1,)),
                dma((4,)),
            ],
            compiler_params=params,
            cost_estimate=pl.CostEstimate(flops=rows * rows * cols, bytes_accessed=4 * rows * cols, transcendentals=0),
        )(l_cols, b_cols)
        return pl.pallas_call(
            functools.partial(finish, side),
            out_shape=jax.ShapeDtypeStruct((rows, cols), jnp.bfloat16),
            in_specs=[pl.BlockSpec(memory_space=pl.ANY)] * 4,
            out_specs=pl.BlockSpec(memory_space=pl.ANY),
            scratch_shapes=[
                pltpu.VMEM((n_copy, blk, cols), jnp.bfloat16),
                pltpu.VMEM((2, per_row * blk, cols), jnp.bfloat16),
                pltpu.VMEM((8, blk, per_row * blk), jnp.bfloat16),
                pltpu.VMEM((4, blk, cols), jnp.float32),
                pltpu.VMEM((4, blk, cols), jnp.bfloat16),
                dma((2,)),
                dma((8,)),
                dma((4,)),
                dma((n_copy,)),
                dma((n_copy + 4,)),
            ],
            compiler_params=pltpu.CompilerParams(vmem_limit_bytes=67043328),
            cost_estimate=pl.CostEstimate(flops=2 * rows * blk * cols, bytes_accessed=6 * rows * cols, transcendentals=0),
        )(strips, partial, gathered, b_cols)

    return jax.shard_map(local_product, mesh=mesh, in_specs=(P("batch", "col"), P("batch", "col")), out_specs=P("batch", "col"), check_vma=False)
```
